128 devices in a mesh: fsdp: 32 (over y_lo, z, x), rep: 4 (over y_hi, core).
Axes of the slice: x: 4, y: 4 (y_hi: 2, y_lo: 2; y = y_hi * 2 + y_lo), z: 4, core: 2. Of those that a mesh axis runs over, the one named last changes fastest.
Arguments:
- video_in: bfloat16 [128, 196, 1024], P(('fsdp', 'rep')), may hold values from -6 to 6
- audio_in: bfloat16 [128, 128, 1024], P(('fsdp', 'rep')), may hold values from -6 to 6
- bottle_in: bfloat16 [128, 8, 1024], P(('fsdp', 'rep')), may hold values from -6 to 6
- video_gain: float32 [1024], replicated, may hold values from 0.5 to 8
- audio_gain: float32 [1024], replicated, may hold values from 0.5 to 8
- video_qkv: bfloat16 [1024, 3072], P('fsdp'), may hold values from -0.18 to 0.18
- video_out: bfloat16 [1024, 1024], P('fsdp'), may hold values from -0.1875 to 0.1875
- audio_qkv: bfloat16 [1024, 3072], P('fsdp'), may hold values from -0.18 to 0.18
- audio_out: bfloat16 [1024, 1024], P('fsdp'), may hold values from -0.1875 to 0.1875
- grad_video: bfloat16 [128, 196, 1024], P(('fsdp', 'rep')), may hold values from -6 to 6
- grad_audio: bfloat16 [128, 128, 1024], P(('fsdp', 'rep')), may hold values from -6 to 6
- grad_bottle: bfloat16 [128, 8, 1024], P(('fsdp', 'rep')), may hold values from -6 to 6
Outputs:
- dvideo_in: bfloat16 [128, 196, 1024], P(('fsdp', 'rep'))
- daudio_in: bfloat16 [128, 128, 1024], P(('fsdp', 'rep'))
- dbottle_in: bfloat16 [128, 8, 1024], P(('fsdp', 'rep'))
- video_qkv_grad: float32 [1024, 3072], P('fsdp')
- video_out_grad: float32 [1024, 1024], P('fsdp')
- audio_qkv_grad: float32 [1024, 3072], P('fsdp')
- audio_out_grad: float32 [1024, 1024], P('fsdp')
- video_gain_grad: float32 [1024], replicated
- audio_gain_grad: float32 [1024], replicated
The draws below stay inside these ranges and needn't reach their ends.
All inputs are finite; a program needn't handle non-finite values.
Results may differ from the reference program's by a relative error of at most 0.025.
Values may be sent and summed in bfloat16 or wider, within the bound.
No kernel may reach another device: no remote copies, remote signals or barrier semaphores. Data moves between devices by JAX's collectives and lax.ppermute only.
A program may use at most 128 MiB of HBM per device.

```python
import jax
import jax.numpy as jnp
from jax import lax

D = 1024
HEAD = 64
TV = 196
TA = 128
NB = 8
CPC = 1
CLIPS = 128


def gain_draw(key):
    return jax.random.uniform(key, (D,), jnp.float32, 0.5, 1.5)


def qkv_draw(key):
    base = jax.random.normal(key, (D, 3 * D), jnp.float32)
    return jnp.clip(base * D ** (-0.5), -0.18, 0.18).astype(jnp.bfloat16)


def draw_video_gain(key, part):
    return gain_draw(jax.random.fold_in(key, 101))


def draw_audio_gain(key, part):
    return gain_draw(jax.random.fold_in(key, 202))


def draw_video_qkv(key, part):
    return qkv_draw(jax.random.fold_in(key, 303))


def draw_audio_qkv(key, part):
    return qkv_draw(jax.random.fold_in(key, 404))


def level_of(key, dims, split, smallest, high):
    loudness = 1.0
    for axis_at, parts in split:
        draws = jax.random.uniform(jax.random.fold_in(jax.random.fold_in(key, 6), axis_at), (parts,), jnp.float32, smallest / len(split), high / len(split))
        loudness = loudness * jnp.repeat(jnp.exp(draws), dims[axis_at] // parts).reshape((-1,) + (1,) * (len(dims) - 1 - axis_at))
    return loudness


def bell_draw(rng, extent, spread, reach, pieces=(), dtype=jnp.bfloat16):
    factor_of = level_of(rng, extent, pieces, -0.22, 0.18) if pieces else 1.0
    entries = jax.random.normal(rng, extent, jnp.float32) * spread * factor_of
    return jnp.minimum(jnp.maximum(entries, -reach), reach).astype(dtype)


def setup_inputs(seed: int = 0) -> dict:
    keys = jax.random.split(jax.random.key(seed), 13)
    return {
        "video_in": bell_draw(keys[0], (CLIPS, TV, D), 1.0, 6.0, ((0, 128),)),
        "audio_in": bell_draw(keys[1], (CLIPS, TA, D), 1.0, 6.0, ((0, 128),)),
        "bottle_in": bell_draw(keys[2], (CLIPS, NB, D), 1.0, 6.0, ((0, 128),)),
        "video_gain": draw_video_gain(jax.random.fold_in(keys[12], 71), 0),
        "audio_gain": draw_audio_gain(jax.random.fold_in(keys[12], 71), 0),
        "video_qkv": draw_video_qkv(jax.random.fold_in(keys[12], 71), 0),
        "video_out": bell_draw(keys[6], (D, D), D ** -0.5, 0.1875, ((0, 32),)),
        "audio_qkv": draw_audio_qkv(jax.random.fold_in(keys[12], 71), 0),
        "audio_out": bell_draw(keys[8], (D, D), D ** -0.5, 0.1875, ((0, 32),)),
        "grad_video": bell_draw(keys[9], (CLIPS, TV, D), 1.0, 6.0, ((0, 128),)),
        "grad_audio": bell_draw(keys[10], (CLIPS, TA, D), 1.0, 6.0, ((0, 128),)),
        "grad_bottle": bell_draw(keys[11], (CLIPS, NB, D), 1.0, 6.0, ((0, 128),)),
    }


def stream(tokens, bottle, gain, w_qkv, w_out, d_tokens, bottle_half):
    f32 = jnp.float32
    bf16 = jnp.bfloat16
    z_rows = jnp.concatenate([tokens, bottle], 0)
    rows = z_rows.shape[0]
    width = z_rows.shape[1]
    zf = z_rows.astype(f32)
    inverse = lax.rsqrt(lax.optimization_barrier(jnp.mean(zf * zf, axis=1, keepdims=True)) + 1e-06)
    normed = zf * inverse
    hidden = (normed * gain).astype(bf16)
    qkv = jnp.dot(hidden, w_qkv, preferred_element_type=f32).astype(bf16)
    scale = HEAD ** (-0.5)
    query = qkv[:, :width].reshape(rows, -1, HEAD).astype(f32)
    keyed = qkv[:, width:2 * width].reshape(rows, -1, HEAD).astype(f32)
    valued = qkv[:, 2 * width:].reshape(rows, -1, HEAD).astype(f32)
    scores = jnp.einsum('shd,thd->hst', query, keyed) * scale
    probs = jax.nn.softmax(scores, axis=-1)
    pb = probs.astype(bf16).astype(f32)
    att = jnp.einsum('hst,thd->shd', pb, valued).reshape(rows, width).astype(bf16)
    d_out = jnp.concatenate([d_tokens.astype(f32), bottle_half], 0)
    dyb = d_out.astype(bf16)
    out_term = jnp.dot(att.T, dyb, preferred_element_type=f32)
    datt = jnp.dot(dyb, w_out.T, preferred_element_type=f32).astype(bf16)
    datt_f = datt.reshape(rows, -1, HEAD).astype(f32)
    dprob = jnp.einsum('shd,thd->hst', datt_f, valued)
    dvalue = jnp.einsum('hst,shd->thd', pb, datt_f)
    dscore = probs * (dprob - lax.optimization_barrier(jnp.sum(probs * dprob, axis=-1, keepdims=True))) * scale
    dsb = dscore.astype(bf16).astype(f32)
    dquery = jnp.einsum('hst,thd->shd', dsb, keyed)
    dkey = jnp.einsum('hst,shd->thd', dsb, query)
    dqkv = jnp.concatenate([dquery.reshape(rows, width), dkey.reshape(rows, width), dvalue.reshape(rows, width)], 1).astype(bf16)
    qkv_term = jnp.dot(hidden.T, dqkv, preferred_element_type=f32)
    dhidden = jnp.dot(dqkv, w_qkv.T, preferred_element_type=f32)
    gain_term = lax.optimization_barrier(jnp.sum(dhidden * normed, axis=0))
    dnorm = dhidden * gain
    d_z = d_out + inverse * (dnorm - normed * lax.optimization_barrier(jnp.mean(dnorm * normed, axis=1, keepdims=True)))
    return (d_z, qkv_term, out_term, gain_term)

def rounded(term):
    return lax.optimization_barrier(term.astype(jnp.bfloat16)).astype(jnp.float32)

def reference(video_in, audio_in, bottle_in, video_gain, audio_gain, video_qkv, video_out, audio_qkv, audio_out, grad_video, grad_audio, grad_bottle):

    def one_clip(carry, item):
        x_video, x_audio, x_bottle, g_video, g_audio, g_bottle = item
        half = g_bottle.astype(jnp.float32) * 0.5
        dz_video, qv, ov, gv = stream(x_video, x_bottle, video_gain, video_qkv, video_out, g_video, half)
        dz_audio, qa, oa, ga = stream(x_audio, x_bottle, audio_gain, audio_qkv, audio_out, g_audio, half)
        carry = (carry[0] + qv, carry[1] + ov, carry[2] + qa, carry[3] + oa, carry[4] + gv, carry[5] + ga)
        outs = (dz_video[:TV].astype(jnp.bfloat16), dz_audio[:TA].astype(jnp.bfloat16), (dz_video[TV:] + dz_audio[TA:]).astype(jnp.bfloat16))
        return (carry, outs)

    def zeros_all():
        return (jnp.zeros((D, 3 * D), jnp.float32), jnp.zeros((D, D), jnp.float32), jnp.zeros((D, 3 * D), jnp.float32), jnp.zeros((D, D), jnp.float32), jnp.zeros((D,), jnp.float32), jnp.zeros((D,), jnp.float32))

    def one_device(carry, group):
        local, outs = lax.scan(one_clip, zeros_all(), group)
        carry = (carry[0] + rounded(local[0]), carry[1] + rounded(local[1]), carry[2] + rounded(local[2]), carry[3] + rounded(local[3]), carry[4] + local[4], carry[5] + local[5])
        return (carry, outs)
    groups = CLIPS // CPC
    items = (video_in, audio_in, bottle_in, grad_video, grad_audio, grad_bottle)
    items = tuple((a.reshape((groups, CPC) + a.shape[1:]) for a in items))
    sums, outs = lax.scan(one_device, zeros_all(), items)
    count = float(CLIPS)
    dv = outs[0].reshape(CLIPS, TV, D)
    da = outs[1].reshape(CLIPS, TA, D)
    db = outs[2].reshape(CLIPS, NB, D)
    return (dv, da, db, sums[0] / count, sums[1] / count, sums[2] / count, sums[3] / count, sums[4] / count, sums[5] / count)
```

```python
import jax
import jax.numpy as jnp
from jax import lax
from jax.experimental import pallas as pl
from jax.experimental.pallas import tpu as pltpu
from jax.sharding import Mesh
from jax.sharding import PartitionSpec as P

HEAD = 64
FSDP = ("fsdp_0", "fsdp_1", "fsdp_2")
FSDP_REP = ("fsdp_0", "fsdp_1", "fsdp_2", "rep_0", "rep_1")

f32 = jnp.float32
bf16 = jnp.bfloat16

RING = 4


def place_of(y, z, x, c):
    return (((y % 2) * RING + z) * RING + x) * 4 + (y // 2) * 2 + c


def pairs(move):
    out = []
    for y in range(RING):
        for z in range(RING):
            for x in range(RING):
                for c in range(2):
                    ny, nz, nx, nc = move(y, z, x, c)
                    out.append((place_of(y, z, x, c), place_of(ny % RING, nz % RING, nx % RING, nc)))
    return out


def send(value, move):
    return lax.ppermute(value, FSDP_REP, pairs(move))


def along_y(step):
    return lambda y, z, x, c: (y + step, z, x, c)


def along_last(step):
    return lambda y, z, x, c: (y, z + step * c, x + step * (1 - c), c)


def along_mid(step):
    return lambda y, z, x, c: (y, z + step * (1 - c), x + step * c, c)


def to_partner(y, z, x, c):
    return (y, z, x, 1 - c)


MID = ((0, 0), (0, 1), (-1, 0), (-1, 1), (1, 0), (1, 1), (2, 0), (2, 1))
LAST = (0, -1, 1, 2)


def block_rows():
    z = lax.axis_index("fsdp_1")
    x = lax.axis_index("fsdp_2")
    c = lax.axis_index("rep_1")
    rows = []
    for last in LAST:
        for mid, half in MID:
            zz = jnp.where(c == 0, z + mid, z + last) % RING
            xx = jnp.where(c == 0, x + last, x + mid) % RING
            rows.append(half * 512 + zz * 128 + xx * 32)
    return jnp.stack(rows).astype(jnp.int32)


def place_body(rows, own, left, right, far_a, far_b, wqkv, wout):
    for i in range(4):
        for j in range(8):
            if i == 3:
                block = far_a[j] if j < 4 else far_b[j - 4]
            else:
                block = (own, left, right)[i][j]
            at = pl.multiple_of(rows[i * 8 + j], 32)
            wqkv[pl.ds(at, 32), :] = block[:, :1536]
            wout[pl.ds(at, 32), :] = block[:, 1536:]


def in_vmem(n):
    return [pl.BlockSpec(memory_space=pltpu.VMEM)] * n


def place(rows, own, left, right, far_a, far_b):
    return pl.pallas_call(
        place_body,
        in_specs=[pl.BlockSpec(memory_space=pltpu.SMEM)] + in_vmem(5),
        out_specs=in_vmem(2),
        out_shape=[
            jax.ShapeDtypeStruct((1024, 1536), bf16),
            jax.ShapeDtypeStruct((1024, 512), bf16),
        ],
        name="place",
    )(rows, own, left, right, far_a, far_b)


def pick_body(rows, gqkv, gout, own, left, right, far):
    for i, dst in enumerate((own, left, right, far)):
        for j in range(8):
            at = pl.multiple_of(rows[i * 8 + j], 32)
            dst[j, :, :1536] = gqkv[pl.ds(at, 32), :]
            dst[j, :, 1536:] = gout[pl.ds(at, 32), :]


def pick(rows, gqkv, gout):
    return pl.pallas_call(
        pick_body,
        in_specs=[pl.BlockSpec(memory_space=pltpu.SMEM)] + in_vmem(2),
        out_specs=in_vmem(4),
        out_shape=[jax.ShapeDtypeStruct((8, 32, 2048), bf16)] * 4,
        name="pick",
    )(rows, gqkv, gout)


def gather_weights(qkv_shard, out_shard, rows, after):
    low = lax.axis_index("fsdp_0")
    c = lax.axis_index("rep_1")
    halves = qkv_shard.reshape(32, 3, 2, 512)
    mine = jnp.where(c == 0, halves[:, :, 0], halves[:, :, 1]).reshape(32, 1536)
    shard = jnp.concatenate([mine, out_shard], 1)
    if after is not None:
        shard, _ = lax.optimization_barrier((shard, after))
    top = send(shard[:16], along_y(1))
    bottom = send(shard[16:], along_y(-1))
    other = jnp.concatenate([top, bottom], 0)
    first = jnp.where(low == 0, shard[:, :1536], other[:, :1536])
    second = jnp.where(low == 0, other[:, :1536], shard[:, :1536])
    outw = jnp.where(low == c, shard[:, 1536:], other[:, 1536:])
    block = jnp.stack(
        [
            jnp.concatenate([first, outw[:, :512]], 1),
            jnp.concatenate([second, outw[:, 512:]], 1),
        ]
    )
    left = send(block, along_mid(1))
    right = send(block, along_mid(-1))
    far_a = send(left[:1], along_mid(1))
    far_b = send(right[1:], along_mid(-1))
    own = jnp.concatenate([block, left, right, far_a, far_b], 0)
    left = send(own, along_last(1))
    right = send(own, along_last(-1))
    far_a = send(left[:4], along_last(1))
    far_b = send(right[4:], along_last(-1))
    wqkv, wout = place(rows, own, left, right, far_a, far_b)
    return wqkv, wout, left


def add(*terms):
    total = terms[0].astype(f32)
    for term in terms[1:]:
        total = total + term.astype(f32)
    return total


def reduce_grads(gqkv, gout, rows, count):
    low = lax.axis_index("fsdp_0")
    c = lax.axis_index("rep_1")
    own, left, right, far = pick(rows, gqkv, gout)
    from_left = send(far[:4], along_last(1))
    from_right = send(far[4:], along_last(-1))
    right = jnp.concatenate([add(right[:4], from_left).astype(bf16), right[4:]], 0)
    left = jnp.concatenate([left[:4], add(left[4:], from_right).astype(bf16)], 0)
    a = send(right, along_last(1))
    b = send(left, along_last(-1))
    part = add(own, a, b).astype(bf16)
    from_left = send(part[6:7], along_mid(1))
    from_right = send(part[7:8], along_mid(-1))
    right = jnp.concatenate([add(part[4:5], from_left).astype(bf16), part[5:6]], 0)
    left = jnp.concatenate([part[2:3], add(part[3:4], from_right).astype(bf16)], 0)
    a = send(right, along_mid(1))
    b = send(left, along_mid(-1))
    part = add(part[0:2], a, b)
    outg = jnp.concatenate([part[0, :, 1536:], part[1, :, 1536:]], 1)
    same = jnp.where(low == 0, part[0, :, :1536], part[1, :, :1536])
    cross = jnp.where(low == 0, part[1, :, :1536], part[0, :, :1536])
    same = jnp.concatenate([same, outg], 1)
    cross = jnp.concatenate([cross, outg], 1).astype(bf16)
    a = send(cross, along_y(1))
    b = send(cross, along_y(-1))
    d = send(same.astype(bf16), along_y(2))
    total = (add(same.astype(bf16), d) + add(a, b)) / count
    peer = send(total, to_partner)
    mine = total[:, :1536].reshape(32, 3, 1, 512)
    other = peer[:, :1536].reshape(32, 3, 1, 512)
    first = jnp.where(c == 0, mine, other)
    second = jnp.where(c == 0, other, mine)
    qkv_grad = jnp.concatenate([first, second], 2).reshape(32, 3072)
    out_grad = jnp.where(low == c, total[:, 1536:], peer[:, 1536:])
    return qkv_grad, out_grad


def all_sum(value):
    steps = [to_partner]
    for bit in (1, 2):
        steps.append(lambda y, z, x, c, bit=bit: (y, z, x ^ bit, c))
        steps.append(lambda y, z, x, c, bit=bit: (y, z ^ bit, x, c))
        steps.append(lambda y, z, x, c, bit=bit: (y ^ bit, z, x, c))
    for step in steps:
        value = value + send(value, step)
    return value


def clip_pair(tokens, bottle, d_tokens, d_bottle):
    z = jnp.concatenate([tokens, bottle], 0)
    half = (d_bottle.astype(f32) * 0.5).astype(bf16)
    dyb = jnp.concatenate([d_tokens, half], 0)
    both = jnp.stack([z, dyb])
    peer = send(both, to_partner)
    return jnp.stack([both, peer])


def stream(zd, gain, wqkv, wout):
    rows = zd.shape[2]
    z = zd[:, 0].astype(f32)
    dyb = zd[:, 1].reshape(2 * rows, 1024)
    inverse = lax.rsqrt(jnp.mean(z * z, axis=2, keepdims=True) + 1e-06)
    normed = z * inverse
    hidden = (normed * gain).astype(bf16).reshape(2 * rows, 1024)
    qkv = jnp.dot(hidden, wqkv, preferred_element_type=f32).astype(bf16)
    scale = HEAD ** (-0.5)
    query = qkv[:, :512].reshape(2, rows, 8, HEAD)
    keyed = qkv[:, 512:1024].reshape(2, rows, 8, HEAD)
    valued = qkv[:, 1024:].reshape(2, rows, 8, HEAD)
    scores = jnp.einsum("bshd,bthd->bhst", query, keyed, preferred_element_type=f32) * scale
    probs = jax.nn.softmax(scores, axis=-1)
    pb = probs.astype(bf16)
    att = (
        jnp.einsum("bhst,bthd->bshd", pb, valued, preferred_element_type=f32)
        .reshape(2 * rows, 512)
        .astype(bf16)
    )
    out_a = jnp.einsum("sd,se->de", att, dyb[:, :512], preferred_element_type=f32)
    out_b = jnp.einsum("sd,se->de", att, dyb[:, 512:], preferred_element_type=f32)
    out_term = jnp.concatenate([out_a.astype(bf16), out_b.astype(bf16)], 0)
    datt = jnp.einsum("se,de->sd", dyb[:, :512], wout[:512], preferred_element_type=f32)
    datt = datt + jnp.einsum("se,de->sd", dyb[:, 512:], wout[512:], preferred_element_type=f32)
    datt = datt.astype(bf16).reshape(2, rows, 8, HEAD)
    dprob = jnp.einsum("bshd,bthd->bhst", datt, valued, preferred_element_type=f32)
    dvalue = jnp.einsum("bhst,bshd->bthd", pb, datt, preferred_element_type=f32)
    dscore = probs * (dprob - jnp.sum(probs * dprob, axis=-1, keepdims=True)) * scale
    dsb = dscore.astype(bf16)
    dquery = jnp.einsum("bhst,bthd->bshd", dsb, keyed, preferred_element_type=f32)
    dkey = jnp.einsum("bhst,bshd->bthd", dsb, query, preferred_element_type=f32)
    dqkv = jnp.concatenate(
        [g.reshape(2 * rows, 512) for g in (dquery, dkey, dvalue)], 1
    ).astype(bf16)
    qkv_term = jnp.einsum("sd,se->de", hidden, dqkv, preferred_element_type=f32).astype(bf16)
    dhidden = jnp.einsum("se,de->sd", dqkv, wqkv, preferred_element_type=f32)
    dhidden = dhidden.reshape(2, rows, 1024)
    dhidden = dhidden[0] + send(dhidden[1], to_partner)
    normed = normed[0]
    gain_term = jnp.sum(dhidden * normed, axis=0)
    dnorm = dhidden * gain
    d_out = zd[0, 1].astype(f32)
    d_z = d_out + inverse[0] * (dnorm - normed * jnp.mean(dnorm * normed, axis=1, keepdims=True))
    return d_z, qkv_term, out_term, gain_term


def per_device(
    video_in,
    audio_in,
    bottle_in,
    video_gain,
    audio_gain,
    video_qkv,
    video_out,
    audio_qkv,
    audio_out,
    grad_video,
    grad_audio,
    grad_bottle,
):
    count = float(video_in.shape[0] * lax.axis_size(FSDP_REP))
    rows = block_rows()
    video_pair = clip_pair(video_in[0], bottle_in[0], grad_video[0], grad_bottle[0])
    audio_pair = clip_pair(audio_in[0], bottle_in[0], grad_audio[0], grad_bottle[0])
    wqkv, wout, mark = gather_weights(video_qkv, video_out, rows, None)
    aqkv, aout, _ = gather_weights(audio_qkv, audio_out, rows, mark)
    dz_video, qkv_term, out_term, gain_v = stream(video_pair, video_gain, wqkv, wout)
    video_qkv_grad, video_out_grad = reduce_grads(qkv_term, out_term, rows, count)
    dz_audio, qkv_term, out_term, gain_a = stream(audio_pair, audio_gain, aqkv, aout)
    audio_qkv_grad, audio_out_grad = reduce_grads(qkv_term, out_term, rows, count)
    gains = all_sum(jnp.stack([gain_v, gain_a])) / count
    video_len = video_in.shape[1]
    audio_len = audio_in.shape[1]
    dvideo_in = dz_video[None, :video_len].astype(bf16)
    daudio_in = dz_audio[None, :audio_len].astype(bf16)
    dbottle_in = (dz_video[None, video_len:] + dz_audio[None, audio_len:]).astype(bf16)
    return (
        dvideo_in,
        daudio_in,
        dbottle_in,
        video_qkv_grad,
        video_out_grad,
        audio_qkv_grad,
        audio_out_grad,
        gains[0],
        gains[1],
    )


def solution(mesh):
    split = Mesh(
        mesh.devices.reshape(2, 4, 4, 2, 2), ("fsdp_0", "fsdp_1", "fsdp_2", "rep_0", "rep_1")
    )
    return jax.shard_map(
        per_device,
        mesh=split,
        in_specs=(
            P(FSDP_REP, None, None),
            P(FSDP_REP, None, None),
            P(FSDP_REP, None, None),
            P(),
            P(),
            P(FSDP, None),
            P(FSDP, None),
            P(FSDP, None),
            P(FSDP, None),
            P(FSDP_REP, None, None),
            P(FSDP_REP, None, None),
            P(FSDP_REP, None, None),
        ),
        out_specs=(
            P(FSDP_REP, None, None),
            P(FSDP_REP, None, None),
            P(FSDP_REP, None, None),
            P(FSDP, None),
            P(FSDP, None),
            P(FSDP, None),
            P(FSDP, None),
            P(),
            P(),
        ),
        check_vma=False,
    )
```

```python
import jax
import jax.numpy as jnp
from jax import lax
from jax.experimental import pallas as pl
from jax.experimental.pallas import tpu as pltpu
from jax.sharding import Mesh
from jax.sharding import PartitionSpec as P

HEAD = 64
FSDP = ("fsdp_0", "fsdp_1", "fsdp_2")
FSDP_REP = ("fsdp_0", "fsdp_1", "fsdp_2", "rep_0", "rep_1")

f32 = jnp.float32
bf16 = jnp.bfloat16

RING = 4


def place_of(y, z, x, c):
    return (((y % 2) * RING + z) * RING + x) * 4 + (y // 2) * 2 + c


def pairs(move):
    out = []
    for y in range(RING):
        for z in range(RING):
            for x in range(RING):
                for c in range(2):
                    ny, nz, nx, nc = move(y, z, x, c)
                    out.append((place_of(y, z, x, c), place_of(ny % RING, nz % RING, nx % RING, nc)))
    return out


def send(value, move):
    return lax.ppermute(value, FSDP_REP, pairs(move))


def along_y(step):
    return lambda y, z, x, c: (y + step, z, x, c)


def along_last(step):
    return lambda y, z, x, c: (y, z + step * c, x + step * (1 - c), c)


def along_mid(step):
    return lambda y, z, x, c: (y, z + step * (1 - c), x + step * c, c)


def to_partner(y, z, x, c):
    return (y, z, x, 1 - c)


MID = ((0, 0), (0, 1), (-1, 0), (-1, 1), (1, 0), (1, 1), (2, 0), (2, 1))
LAST = (0, -1, 1, 2)


def block_rows():
    z = lax.axis_index("fsdp_1")
    x = lax.axis_index("fsdp_2")
    c = lax.axis_index("rep_1")
    rows = []
    for last in LAST:
        for mid, half in MID:
            zz = jnp.where(c == 0, z + mid, z + last) % RING
            xx = jnp.where(c == 0, x + last, x + mid) % RING
            rows.append(half * 512 + zz * 128 + xx * 32)
    rows.append(c * 512)
    return jnp.stack(rows).astype(jnp.int32)


def in_vmem(n):
    return [pl.BlockSpec(memory_space=pltpu.VMEM)] * n


def in_smem():
    return pl.BlockSpec(memory_space=pltpu.SMEM)


def dot_nn(a, b):
    return lax.dot_general(a, b, (((1,), (0,)), ((), ())), preferred_element_type=f32)


def dot_nt(a, b):
    return lax.dot_general(a, b, (((1,), (1,)), ((), ())), preferred_element_type=f32)


def dot_tn(a, b):
    return lax.dot_general(a, b, (((0,), (0,)), ((), ())), preferred_element_type=f32)


def local_body(length, placed, rows, own, peer, gain, *refs):
    size = own.shape[1]
    n_weights = 1 if placed else 20
    weights, refs = refs[:n_weights], refs[n_weights:]
    grads, refs = refs[:7], refs[7:]
    dh, refs = refs[0], refs[1:]
    hidden, dyb, qkv, datt, att, dqkv, gqkv, gout, wqkv, wout = refs

    if placed:
        (full,) = weights
        base = pl.multiple_of(rows[32], 512)

        def w_qkv(n):
            top = pl.multiple_of((n // 5) * 1024, 1024)
            return full[pl.ds(top, 1024), pl.ds(pl.multiple_of((n % 5) * 256, 256), 256)]

        def w_out(half):
            return full[pl.ds(1024 + base, 512), 256 + 512 * half : 768 + 512 * half]
    else:
        for n, ref in enumerate(weights):
            for k in range(ref.shape[0]):
                at = pl.multiple_of(rows[PIECE_BLOCKS[n][k]], 32)
                wqkv[pl.ds(at, 32), :] = ref[k, :, :1536]
                wout[pl.ds(at, 32), :] = ref[k, :, 1536:]

        def w_qkv(n):
            return wqkv[:, pl.ds(pl.multiple_of(n * 256, 256), 256)]

        def w_out(half):
            return wout[512 * half : 512 * half + 512, :]

    for b, pair in enumerate((own, peer)):
        z = pair[0].astype(f32)
        inverse = lax.rsqrt(jnp.mean(z * z, axis=1, keepdims=True) + 1e-06)
        hidden[b * size : (b + 1) * size, :] = (z * inverse * gain[...]).astype(bf16)
        dyb[b * size : (b + 1) * size, :] = pair[1]

    @pl.loop(0, 6)
    def _(n):
        at = pl.multiple_of(n * 256, 256)
        qkv[:, pl.ds(at, 256)] = dot_nn(hidden[...], w_qkv(n)).astype(bf16)

    datt[...] = (dot_nt(dyb[:, :512], w_out(0)) + dot_nt(dyb[:, 512:], w_out(1))).astype(bf16)

    scale = HEAD ** (-0.5)
    lane = lax.broadcasted_iota(jnp.int32, (size, 128), 1)
    key_at = lax.broadcasted_iota(jnp.int32, (size, size), 1)
    zero = jnp.zeros((), bf16)

    @pl.loop(0, 8)
    def _(n):
        r = pl.ds(pl.multiple_of((n // 4) * size, 16), size)
        at = pl.multiple_of((n % 4) * 128, 128)
        query = qkv[r, pl.ds(at, 128)]
        keyed = qkv[r, pl.ds(at + 512, 128)]
        valued = qkv[r, pl.ds(at + 1024, 128)]
        dout = datt[r, pl.ds(at, 128)]
        sums = [None] * 4
        for head in range(2):
            mine = (lane < HEAD) if head == 0 else (lane >= HEAD)
            q = jnp.where(mine, query, zero)
            k = jnp.where(mine, keyed, zero)
            v = jnp.where(mine, valued, zero)
            d = jnp.where(mine, dout, zero)
            score = dot_nt(q, keyed) * scale
            score = jnp.where(key_at < length, score, -1e30)
            top = jnp.max(score, axis=1, keepdims=True)
            grown = jnp.exp(score - top)
            probs = grown * (1.0 / jnp.sum(grown, axis=1, keepdims=True))
            pb = probs.astype(bf16)
            dprob = dot_nt(d, valued)
            inner = jnp.sum(probs * dprob, axis=1, keepdims=True)
            dsb = (probs * (dprob - inner) * scale).astype(bf16)
            parts = (dot_nn(pb, v), dot_nn(dsb, k), dot_tn(dsb, q), dot_tn(pb, d))
            sums = [p if t is None else t + p for t, p in zip(sums, parts)]
        att[r, pl.ds(at, 128)] = sums[0].astype(bf16)
        dqkv[r, pl.ds(at, 128)] = sums[1].astype(bf16)
        dqkv[r, pl.ds(at + 512, 128)] = sums[2].astype(bf16)
        dqkv[r, pl.ds(at + 1024, 128)] = sums[3].astype(bf16)

    for half in range(2):
        gout[512 * half : 512 * half + 512, :] = dot_tn(
            att[...], dyb[:, 512 * half : 512 * half + 512]
        ).astype(bf16)

    @pl.loop(0, 6)
    def _(n):
        at = pl.multiple_of(n * 256, 256)
        gqkv[:, pl.ds(at, 256)] = dot_tn(hidden[...], dqkv[:, pl.ds(at, 256)]).astype(bf16)

    for n, ref in enumerate(grads):
        for k in range(ref.shape[0]):
            at = pl.multiple_of(rows[GRAD_BLOCKS[n][k]], 32)
            ref[k, :, :1536] = gqkv[pl.ds(at, 32), :]
            ref[k, :, 1536:] = gout[pl.ds(at, 32), :]

    @pl.loop(0, 2)
    def _(n):
        r = pl.ds(pl.multiple_of(n * size, 16), size)
        total = jnp.zeros((size, 1024), f32)
        for k in range(6):
            total = total + dot_nt(dqkv[r, k * 256 : k * 256 + 256], w_qkv(k))
        dh[n] = total


PIECE_BLOCKS = []
for start in (0, 8, 16):
    PIECE_BLOCKS += [(start, start + 1), (start + 2, start + 3), (start + 4, start + 5), (start + 6,), (start + 7,)]
PIECE_BLOCKS += [(24, 25), (26, 27), (28, 29), (30,), (31,)]
GRAD_BLOCKS = [tuple(range(8))]
for start in (8, 16, 24):
    GRAD_BLOCKS += [tuple(range(start, start + 4)), tuple(range(start + 4, start + 8))]


def local_compute(length, placed, rows, own, peer, gain, weights):
    size = own.shape[1]
    total = 2 * size
    return pl.pallas_call(
        lambda *refs: local_body(length, placed, *refs),
        in_specs=[in_smem()] + in_vmem(3 + len(weights)),
        out_specs=in_vmem(8),
        out_shape=[jax.ShapeDtypeStruct((8, 32, 2048), bf16)]
        + [jax.ShapeDtypeStruct((4, 32, 2048), bf16)] * 6
        + [jax.ShapeDtypeStruct((2, size, 1024), f32)],
        scratch_shapes=[
            pltpu.VMEM((total, 1024), bf16),
            pltpu.VMEM((total, 1024), bf16),
            pltpu.VMEM((total, 1536), bf16),
            pltpu.VMEM((total, 512), bf16),
            pltpu.VMEM((total, 512), bf16),
            pltpu.VMEM((total, 1536), bf16),
            pltpu.VMEM((1024, 1536), bf16),
            pltpu.VMEM((1024, 512), bf16),
            pltpu.VMEM((16 if placed else 1024, 1536), bf16),
            pltpu.VMEM((16 if placed else 1024, 512), bf16),
        ],
        name="local_placed" if placed else "local_pieces",
    )(rows, own, peer, gain.reshape(1, 1024), *weights)


def my_columns(qkv_shard):
    c = lax.axis_index("rep_1")
    halves = qkv_shard.reshape(32, 3, 2, 512)
    return jnp.where(c == 0, halves[:, :, 0], halves[:, :, 1]).reshape(32, 1536)


def gather_by_calls(qkv_shard, out_shard):
    high = lax.axis_index("rep_0")
    shard = jnp.concatenate([my_columns(qkv_shard), out_shard], 1)
    shard = jnp.where(high == 0, shard[:, :1280], shard[:, 1280:])
    return lax.all_gather(shard, ("rep_0",) + FSDP, axis=0, tiled=True)


def gather_by_rings(qkv_shard, out_shard):
    low = lax.axis_index("fsdp_0")
    c = lax.axis_index("rep_1")
    shard = jnp.concatenate([my_columns(qkv_shard), out_shard], 1)
    top = send(shard[:16], along_y(1))
    bottom = send(shard[16:], along_y(-1))
    other = jnp.concatenate([top, bottom], 0)
    first = jnp.where(low == 0, shard[:, :1536], other[:, :1536])
    second = jnp.where(low == 0, other[:, :1536], shard[:, :1536])
    outw = jnp.where(low == c, shard[:, 1536:], other[:, 1536:])
    block = jnp.stack(
        [
            jnp.concatenate([first, outw[:, :512]], 1),
            jnp.concatenate([second, outw[:, 512:]], 1),
        ]
    )
    left = send(block, along_mid(1))
    right = send(block, along_mid(-1))
    far_a = send(left[:1], along_mid(1))
    far_b = send(right[1:], along_mid(-1))
    own = [block, left, right, far_a, far_b]
    from_left = [send(piece, along_last(1)) for piece in own]
    from_right = [send(piece, along_last(-1)) for piece in own]
    across = [send(piece, along_last(1)) for piece in from_left[:2]]
    across += [send(piece, along_last(-1)) for piece in from_right[2:]]
    return own + from_left + from_right + across


def add(*terms):
    total = terms[0].astype(f32)
    for term in terms[1:]:
        total = total + term.astype(f32)
    return total


def reduce_grads(grads, count):
    low = lax.axis_index("fsdp_0")
    c = lax.axis_index("rep_1")
    own, left_a, left_b, right_a, right_b, far_a, far_b = grads
    up_far = send(far_a, along_last(1))
    down_far = send(far_b, along_last(-1))
    up_b = send(right_b, along_last(1))
    down_a = send(left_a, along_last(-1))
    up_a = send(add(right_a, up_far).astype(bf16), along_last(1))
    down_b = send(add(left_b, down_far).astype(bf16), along_last(-1))
    part_b = add(own[4:], up_b, down_b).astype(bf16)
    part_a = add(own[:4], up_a, down_a).astype(bf16)
    up_far = send(part_b[2], along_mid(1))
    down_far = send(part_b[3], along_mid(-1))
    up_b = send(part_b[1], along_mid(1))
    down_a = send(part_a[2], along_mid(-1))
    up_a = send(add(part_b[0], up_far).astype(bf16), along_mid(1))
    down_b = send(add(part_a[3], down_far).astype(bf16), along_mid(-1))
    first = add(part_a[0], up_a, down_a)
    second = add(part_a[1], up_b, down_b)
    outg = jnp.concatenate([first[:, 1536:], second[:, 1536:]], 1)
    first, second = first[:, :1536], second[:, :1536]
    same = jnp.where(low == 0, first, second)
    cross = jnp.where(low == 0, second, first)
    same = jnp.concatenate([same, outg], 1).astype(bf16)
    cross = jnp.concatenate([cross, outg], 1).astype(bf16)
    a = send(cross, along_y(1))
    b = send(cross, along_y(-1))
    d = send(same, along_y(2))
    total = (add(same, d) + add(a, b)) / count
    peer = send(total, to_partner)
    mine = total[:, :1536].reshape(32, 3, 1, 512)
    other = peer[:, :1536].reshape(32, 3, 1, 512)
    first = jnp.where(c == 0, mine, other)
    second = jnp.where(c == 0, other, mine)
    qkv_grad = jnp.concatenate([first, second], 2).reshape(32, 3072)
    out_grad = jnp.where(low == c, total[:, 1536:], peer[:, 1536:])
    return qkv_grad, out_grad


def all_sum(value):
    for along in (along_last, along_mid, along_y):
        near = send(value, along(1)) + send(value, along(-1))
        value = (value + send(value, along(2))) + near
    return value + send(value, to_partner)


def clip_pair(tokens, bottle, d_tokens, d_bottle):
    half = (d_bottle.astype(f32) * 0.5).astype(bf16)
    pad = jnp.zeros((-(tokens.shape[0] + bottle.shape[0]) % 16, 1024), bf16)
    own = jnp.stack(
        [jnp.concatenate([tokens, bottle, pad], 0), jnp.concatenate([d_tokens, half, pad], 0)]
    )
    return own, send(own, to_partner)


def finish(own, gain, dh):
    dhidden = dh[0] + send(dh[1], to_partner)
    z = own[0].astype(f32)
    inverse = lax.rsqrt(jnp.mean(z * z, axis=1, keepdims=True) + 1e-06)
    normed = z * inverse
    gain_term = jnp.sum(dhidden * normed, axis=0)
    dnorm = dhidden * gain
    d_out = own[1].astype(f32)
    d_z = d_out + inverse * (dnorm - normed * jnp.mean(dnorm * normed, axis=1, keepdims=True))
    return d_z, gain_term


def per_device(
    video_in,
    audio_in,
    bottle_in,
    video_gain,
    audio_gain,
    video_qkv,
    video_out,
    audio_qkv,
    audio_out,
    grad_video,
    grad_audio,
    grad_bottle,
):
    count = float(video_in.shape[0] * lax.axis_size(FSDP_REP))
    rows = block_rows()
    video_len = video_in.shape[1]
    audio_len = audio_in.shape[1]
    bottle_len = bottle_in.shape[1]
    aweights = gather_by_calls(audio_qkv, audio_out)
    vweights = gather_by_rings(video_qkv, video_out)
    vown, vpeer = clip_pair(video_in[0], bottle_in[0], grad_video[0], grad_bottle[0])
    aown, apeer = clip_pair(audio_in[0], bottle_in[0], grad_audio[0], grad_bottle[0])
    *grads, dh = local_compute(
        video_len + bottle_len, False, rows, vown, vpeer, video_gain, vweights
    )
    video_qkv_grad, video_out_grad = reduce_grads(grads, count)
    dz_video, gain_v = finish(vown, video_gain, dh)
    *grads, dh = local_compute(
        audio_len + bottle_len, True, rows, aown, apeer, audio_gain, [aweights]
    )
    audio_qkv_grad, audio_out_grad = reduce_grads(grads, count)
    dz_audio, gain_a = finish(aown, audio_gain, dh)
    gains = all_sum(jnp.stack([gain_v, gain_a])) / count
    video_end = video_len + bottle_len
    audio_end = audio_len + bottle_len
    dvideo_in = dz_video[None, :video_len].astype(bf16)
    daudio_in = dz_audio[None, :audio_len].astype(bf16)
    dbottle_in = dz_video[None, video_len:video_end] + dz_audio[None, audio_len:audio_end]
    dbottle_in = dbottle_in.astype(bf16)
    return (
        dvideo_in,
        daudio_in,
        dbottle_in,
        video_qkv_grad,
        video_out_grad,
        audio_qkv_grad,
        audio_out_grad,
        gains[0],
        gains[1],
    )


def solution(mesh):
    split = Mesh(
        mesh.devices.reshape(2, 4, 4, 2, 2), ("fsdp_0", "fsdp_1", "fsdp_2", "rep_0", "rep_1")
    )
    return jax.shard_map(
        per_device,
        mesh=split,
        in_specs=(
            P(FSDP_REP, None, None),
            P(FSDP_REP, None, None),
            P(FSDP_REP, None, None),
            P(),
            P(),
            P(FSDP, None),
            P(FSDP, None),
            P(FSDP, None),
            P(FSDP, None),
            P(FSDP_REP, None, None),
            P(FSDP_REP, None, None),
            P(FSDP_REP, None, None),
        ),
        out_specs=(
            P(FSDP_REP, None, None),
            P(FSDP_REP, None, None),
            P(FSDP_REP, None, None),
            P(FSDP, None),
            P(FSDP, None),
            P(FSDP, None),
            P(FSDP, None),
            P(),
            P(),
        ),
        check_vma=False,
    )
```

```python
import jax
import jax.numpy as jnp
from jax import lax
from jax.experimental import pallas as pl
from jax.experimental.pallas import tpu as pltpu
from jax.sharding import Mesh
from jax.sharding import PartitionSpec as P

HEAD = 64
FSDP = ("fsdp_0", "fsdp_1", "fsdp_2")
FSDP_REP = ("fsdp_0", "fsdp_1", "fsdp_2", "rep_0", "rep_1")

f32 = jnp.float32
bf16 = jnp.bfloat16

RING = 4


def place_of(y, z, x, c):
    return (((y % 2) * RING + z) * RING + x) * 4 + (y // 2) * 2 + c


def pairs(move):
    out = []
    for y in range(RING):
        for z in range(RING):
            for x in range(RING):
                for c in range(2):
                    ny, nz, nx, nc = move(y, z, x, c)
                    out.append((place_of(y, z, x, c), place_of(ny % RING, nz % RING, nx % RING, nc)))
    return out


def send(value, move):
    return lax.ppermute(value, FSDP_REP, pairs(move))


def along_y(step):
    return lambda y, z, x, c: (y + step, z, x, c)


def along_last(step):
    return lambda y, z, x, c: (y, z + step * c, x + step * (1 - c), c)


def along_mid(step):
    return lambda y, z, x, c: (y, z + step * (1 - c), x + step * c, c)


def to_partner(y, z, x, c):
    return (y, z, x, 1 - c)


MID = ((0, 0), (0, 1), (-1, 0), (-1, 1), (1, 0), (1, 1), (2, 0), (2, 1))
LAST = (0, -1, 1, 2)


def coordinates():
    return jnp.stack([lax.axis_index(name) for name in ("fsdp_1", "fsdp_2", "rep_1")]).astype(jnp.int32)


def block_row(where, block):
    z, x, c = where[0], where[1], where[2]
    last = LAST[block // 8]
    mid, half = MID[block % 8]
    zz = (z + mid * (1 - c) + last * c) & (RING - 1)
    xx = (x + last * (1 - c) + mid * c) & (RING - 1)
    return pl.multiple_of(half * 512 + zz * 128 + xx * 32, 32)


def in_vmem(n):
    return [pl.BlockSpec(memory_space=pltpu.VMEM)] * n


def in_smem():
    return pl.BlockSpec(memory_space=pltpu.SMEM)


def dot_nn(a, b):
    return lax.dot_general(a, b, (((1,), (0,)), ((), ())), preferred_element_type=f32)


def dot_nt(a, b):
    return lax.dot_general(a, b, (((1,), (1,)), ((), ())), preferred_element_type=f32)


def dot_tn(a, b):
    return lax.dot_general(a, b, (((0,), (0,)), ((), ())), preferred_element_type=f32)


def local_body(length, placed, where, own, peer, gain, *refs):
    size = own.shape[1]
    n_weights = 1 if placed else 20
    weights, refs = refs[:n_weights], refs[n_weights:]
    grads, refs = refs[:7], refs[7:]
    dh, gain_part, refs = refs[0], refs[1], refs[2:]
    hidden, hidden_t, dyb, qkv, datt, att, dqkv, gqkv, gout, wqkv, wout = refs

    if placed:
        (full,) = weights
        base = pl.multiple_of(where[2] * 512, 512)

        def w_qkv(n):
            top = pl.multiple_of((n // 5) * 1024, 1024)
            return full[pl.ds(top, 1024), pl.ds(pl.multiple_of((n % 5) * 256, 256), 256)]

        def w_out(half):
            return full[pl.ds(1024 + base, 512), 256 + 512 * half : 768 + 512 * half]
    else:
        for n, ref in enumerate(weights):
            for k in range(ref.shape[0]):
                at = block_row(where, PIECE_BLOCKS[n][k])
                wqkv[pl.ds(at, 32), :] = ref[k, :, :1536]
                wout[pl.ds(at, 32), :] = ref[k, :, 1536:]

        def w_qkv(n):
            return wqkv[:, pl.ds(pl.multiple_of(n * 256, 256), 256)]

        def w_out(half):
            return wout[512 * half : 512 * half + 512, :]

    for b, pair in enumerate((own, peer)):
        z = pair[0].astype(f32)
        inverse = lax.rsqrt(jnp.mean(z * z, axis=1, keepdims=True) + 1e-06)
        hidden[b * size : (b + 1) * size, :] = (z * inverse * gain[...]).astype(bf16)
        dyb[b * size : (b + 1) * size, :] = pair[1]
    hidden_t[...] = hidden[...].T

    @pl.loop(0, 6)
    def _(n):
        at = pl.multiple_of(n * 256, 256)
        qkv[:, pl.ds(at, 256)] = dot_nn(hidden[...], w_qkv(n)).astype(bf16)

    datt[...] = (dot_nt(dyb[:, :512], w_out(0)) + dot_nt(dyb[:, 512:], w_out(1))).astype(bf16)

    scale = HEAD ** (-0.5)
    lane = lax.broadcasted_iota(jnp.int32, (size, 128), 1)
    key_at = lax.broadcasted_iota(jnp.int32, (size, size), 1)
    zero = jnp.zeros((), bf16)

    @pl.loop(0, 8)
    def _(n):
        r = pl.ds(pl.multiple_of((n // 4) * size, 16), size)
        at = pl.multiple_of((n % 4) * 128, 128)
        query = qkv[r, pl.ds(at, 128)]
        keyed = qkv[r, pl.ds(at + 512, 128)]
        valued = qkv[r, pl.ds(at + 1024, 128)]
        dout = datt[r, pl.ds(at, 128)]
        sums = [None] * 4
        for head in range(2):
            mine = (lane < HEAD) if head == 0 else (lane >= HEAD)
            q = jnp.where(mine, query, zero)
            k = jnp.where(mine, keyed, zero)
            v = jnp.where(mine, valued, zero)
            d = jnp.where(mine, dout, zero)
            score = dot_nt(q, keyed) * scale
            score = jnp.where(key_at < length, score, -1e30)
            top = jnp.max(score, axis=1, keepdims=True)
            grown = jnp.exp(score - top)
            probs = grown * (1.0 / jnp.sum(grown, axis=1, keepdims=True))
            pb = probs.astype(bf16)
            dprob = dot_nt(d, valued)
            inner = jnp.sum(probs * dprob, axis=1, keepdims=True)
            dsb = (probs * (dprob - inner) * scale).astype(bf16)
            parts = (dot_nn(pb, v), dot_nn(dsb, k), dot_tn(dsb, q), dot_tn(pb, d))
            sums = [p if t is None else t + p for t, p in zip(sums, parts)]
        att[r, pl.ds(at, 128)] = sums[0].astype(bf16)
        dqkv[r, pl.ds(at, 128)] = sums[1].astype(bf16)
        dqkv[r, pl.ds(at + 512, 128)] = sums[2].astype(bf16)
        dqkv[r, pl.ds(at + 1024, 128)] = sums[3].astype(bf16)

    att_t = att[...].T
    for half in range(2):
        gout[512 * half : 512 * half + 512, :] = dot_nn(
            att_t, dyb[:, 512 * half : 512 * half + 512]
        ).astype(bf16)

    @pl.loop(0, 6)
    def _(n):
        at = pl.multiple_of(n * 256, 256)
        gqkv[:, pl.ds(at, 256)] = dot_nn(hidden_t[...], dqkv[:, pl.ds(at, 256)]).astype(bf16)

    for n, ref in enumerate(grads):
        for k in range(ref.shape[0]):
            at = block_row(where, GRAD_BLOCKS[n][k])
            ref[k, :, :1536] = gqkv[pl.ds(at, 32), :]
            ref[k, :, 1536:] = gout[pl.ds(at, 32), :]

    part = jnp.zeros((1, 1024), f32)
    for b, pair in enumerate((own, peer)):
        total = dot_nt(dqkv[b * size : (b + 1) * size, :256], w_qkv(0))
        for k in range(1, 6):
            total = total + dot_nt(dqkv[b * size : (b + 1) * size, k * 256 : k * 256 + 256], w_qkv(k))
        dh[b] = total
        z = pair[0].astype(f32)
        normed = z * lax.rsqrt(jnp.mean(z * z, axis=1, keepdims=True) + 1e-06)
        part = part + jnp.sum(total * normed, axis=0, keepdims=True)
    gain_part[...] = part


PIECE_BLOCKS = []
for start in (0, 8, 16):
    PIECE_BLOCKS += [(start, start + 1), (start + 2, start + 3), (start + 4, start + 5), (start + 6,), (start + 7,)]
PIECE_BLOCKS += [(24, 25), (26, 27), (28, 29), (30,), (31,)]
GRAD_BLOCKS = [tuple(range(8))]
for start in (8, 16, 24):
    GRAD_BLOCKS += [tuple(range(start, start + 4)), tuple(range(start + 4, start + 8))]


def local_compute(length, placed, where, own, peer, gain, weights):
    size = own.shape[1]
    total = 2 * size
    return pl.pallas_call(
        lambda *refs: local_body(length, placed, *refs),
        in_specs=[in_smem()] + in_vmem(3 + len(weights)),
        out_specs=in_vmem(9),
        out_shape=[jax.ShapeDtypeStruct((8, 32, 2048), bf16)]
        + [jax.ShapeDtypeStruct((4, 32, 2048), bf16)] * 6
        + [jax.ShapeDtypeStruct((2, size, 1024), f32), jax.ShapeDtypeStruct((1, 1024), f32)],
        scratch_shapes=[
            pltpu.VMEM((total, 1024), bf16),
            pltpu.VMEM((1024, total), bf16),
            pltpu.VMEM((total, 1024), bf16),
            pltpu.VMEM((total, 1536), bf16),
            pltpu.VMEM((total, 512), bf16),
            pltpu.VMEM((total, 512), bf16),
            pltpu.VMEM((total, 1536), bf16),
            pltpu.VMEM((1024, 1536), bf16),
            pltpu.VMEM((1024, 512), bf16),
            pltpu.VMEM((16 if placed else 1024, 1536), bf16),
            pltpu.VMEM((16 if placed else 1024, 512), bf16),
        ],
        name="local_placed" if placed else "local_pieces",
    )(where, own, peer, gain.reshape(1, 1024), *weights)


def my_columns(qkv_shard):
    c = lax.axis_index("rep_1")
    halves = qkv_shard.reshape(32, 3, 2, 512)
    return jnp.where(c == 0, halves[:, :, 0], halves[:, :, 1]).reshape(32, 1536)


def gather_by_calls(qkv_shard, out_shard):
    high = lax.axis_index("rep_0")
    shard = jnp.concatenate([my_columns(qkv_shard), out_shard], 1)
    shard = jnp.where(high == 0, shard[:, :1280], shard[:, 1280:])
    return lax.all_gather(shard, ("rep_0",) + FSDP, axis=0, tiled=True)


def gather_by_rings(qkv_shard, out_shard):
    low = lax.axis_index("fsdp_0")
    c = lax.axis_index("rep_1")
    shard = jnp.concatenate([my_columns(qkv_shard), out_shard], 1)
    top = send(shard[:16], along_y(1))
    bottom = send(shard[16:], along_y(-1))
    other = jnp.concatenate([top, bottom], 0)
    first = jnp.where(low == 0, shard[:, :1536], other[:, :1536])
    second = jnp.where(low == 0, other[:, :1536], shard[:, :1536])
    outw = jnp.where(low == c, shard[:, 1536:], other[:, 1536:])
    block = jnp.stack(
        [
            jnp.concatenate([first, outw[:, :512]], 1),
            jnp.concatenate([second, outw[:, 512:]], 1),
        ]
    )
    left = send(block, along_mid(1))
    right = send(block, along_mid(-1))
    far_a = send(left[:1], along_mid(1))
    far_b = send(right[1:], along_mid(-1))
    own = [block, left, right, far_a, far_b]
    from_left = [send(piece, along_last(1)) for piece in own]
    from_right = [send(piece, along_last(-1)) for piece in own]
    across = [send(piece, along_last(1)) for piece in from_left[:2]]
    across += [send(piece, along_last(-1)) for piece in from_right[2:]]
    return own + from_left + from_right + across


def add(*terms):
    total = terms[0].astype(f32)
    for term in terms[1:]:
        total = total + term.astype(f32)
    return total


def reduce_grads(grads, count):
    low = lax.axis_index("fsdp_0")
    c = lax.axis_index("rep_1")
    own, left_a, left_b, right_a, right_b, far_a, far_b = grads
    up_far = send(far_a, along_last(1))
    down_far = send(far_b, along_last(-1))
    up_b = send(right_b, along_last(1))
    down_a = send(left_a, along_last(-1))
    up_a = send(add(right_a, up_far).astype(bf16), along_last(1))
    down_b = send(add(left_b, down_far).astype(bf16), along_last(-1))
    part_b = add(own[4:], up_b, down_b).astype(bf16)
    part_a = add(own[:4], up_a, down_a).astype(bf16)
    up_far = send(part_b[2], along_mid(1))
    down_far = send(part_b[3], along_mid(-1))
    up_b = send(part_b[1], along_mid(1))
    down_a = send(part_a[2], along_mid(-1))
    up_a = send(add(part_b[0], up_far).astype(bf16), along_mid(1))
    down_b = send(add(part_a[3], down_far).astype(bf16), along_mid(-1))
    first = add(part_a[0], up_a, down_a)
    second = add(part_a[1], up_b, down_b)
    outg = jnp.concatenate([first[:, 1536:], second[:, 1536:]], 1)
    first, second = first[:, :1536], second[:, :1536]
    same = jnp.where(low == 0, first, second)
    cross = jnp.where(low == 0, second, first)
    same = jnp.concatenate([same, outg], 1).astype(bf16)
    cross = jnp.concatenate([cross, outg], 1).astype(bf16)
    a = send(cross, along_y(1))
    b = send(cross, along_y(-1))
    d = send(same, along_y(2))
    total = (add(same, d) + add(a, b)) / count
    peer = send(total, to_partner)
    mine = total[:, :1536].reshape(32, 3, 1, 512)
    other = peer[:, :1536].reshape(32, 3, 1, 512)
    first = jnp.where(c == 0, mine, other)
    second = jnp.where(c == 0, other, mine)
    qkv_grad = jnp.concatenate([first, second], 2).reshape(32, 3072)
    out_grad = jnp.where(low == c, total[:, 1536:], peer[:, 1536:])
    return qkv_grad, out_grad


def all_sum(value):
    for along in (along_last, along_mid, along_y):
        near = send(value, along(1)) + send(value, along(-1))
        value = (value + send(value, along(2))) + near
    return value + send(value, to_partner)


def clip_pair(tokens, bottle, d_tokens, d_bottle):
    half = (d_bottle.astype(f32) * 0.5).astype(bf16)
    pad = jnp.zeros((-(tokens.shape[0] + bottle.shape[0]) % 16, 1024), bf16)
    own = jnp.stack(
        [jnp.concatenate([tokens, bottle, pad], 0), jnp.concatenate([d_tokens, half, pad], 0)]
    )
    return own, send(own, to_partner)


def finish(own, gain, dh):
    dhidden = dh[0] + send(dh[1], to_partner)
    z = own[0].astype(f32)
    inverse = lax.rsqrt(jnp.mean(z * z, axis=1, keepdims=True) + 1e-06)
    normed = z * inverse
    dnorm = dhidden * gain
    d_out = own[1].astype(f32)
    d_z = d_out + inverse * (dnorm - normed * jnp.mean(dnorm * normed, axis=1, keepdims=True))
    return d_z


def per_device(
    video_in,
    audio_in,
    bottle_in,
    video_gain,
    audio_gain,
    video_qkv,
    video_out,
    audio_qkv,
    audio_out,
    grad_video,
    grad_audio,
    grad_bottle,
):
    count = float(video_in.shape[0] * lax.axis_size(FSDP_REP))
    where = coordinates()
    video_len = video_in.shape[1]
    audio_len = audio_in.shape[1]
    bottle_len = bottle_in.shape[1]
    aweights = gather_by_calls(audio_qkv, audio_out)
    vweights = gather_by_rings(video_qkv, video_out)
    vown, vpeer = clip_pair(video_in[0], bottle_in[0], grad_video[0], grad_bottle[0])
    aown, apeer = clip_pair(audio_in[0], bottle_in[0], grad_audio[0], grad_bottle[0])
    vpeer, apeer = lax.optimization_barrier((vpeer, apeer))
    *grads, dh_video, gain_v = local_compute(
        video_len + bottle_len, False, where, vown, vpeer, video_gain, vweights
    )
    video_qkv_grad, video_out_grad = reduce_grads(grads, count)
    *grads, dh_audio, gain_a = local_compute(
        audio_len + bottle_len, True, where, aown, apeer, audio_gain, [aweights]
    )
    audio_qkv_grad, audio_out_grad = reduce_grads(grads, count)
    gains = all_sum(jnp.concatenate([gain_v, gain_a], 0)) / count
    dz_video = finish(vown, video_gain, dh_video)
    dz_audio = finish(aown, audio_gain, dh_audio)
    video_end = video_len + bottle_len
    audio_end = audio_len + bottle_len
    dvideo_in = dz_video[None, :video_len].astype(bf16)
    daudio_in = dz_audio[None, :audio_len].astype(bf16)
    dbottle_in = dz_video[None, video_len:video_end] + dz_audio[None, audio_len:audio_end]
    dbottle_in = dbottle_in.astype(bf16)
    return (
        dvideo_in,
        daudio_in,
        dbottle_in,
        video_qkv_grad,
        video_out_grad,
        audio_qkv_grad,
        audio_out_grad,
        gains[0],
        gains[1],
    )


def solution(mesh):
    split = Mesh(
        mesh.devices.reshape(2, 4, 4, 2, 2), ("fsdp_0", "fsdp_1", "fsdp_2", "rep_0", "rep_1")
    )
    return jax.shard_map(
        per_device,
        mesh=split,
        in_specs=(
            P(FSDP_REP, None, None),
            P(FSDP_REP, None, None),
            P(FSDP_REP, None, None),
            P(),
            P(),
            P(FSDP, None),
            P(FSDP, None),
            P(FSDP, None),
            P(FSDP, None),
            P(FSDP_REP, None, None),
            P(FSDP_REP, None, None),
            P(FSDP_REP, None, None),
        ),
        out_specs=(
            P(FSDP_REP, None, None),
            P(FSDP_REP, None, None),
            P(FSDP_REP, None, None),
            P(FSDP, None),
            P(FSDP, None),
            P(FSDP, None),
            P(FSDP, None),
            P(),
            P(),
        ),
        check_vma=False,
    )
```

```python
import functools

import jax
import jax.numpy as jnp
from jax import lax
from jax.experimental import pallas as pl
from jax.experimental.pallas import tpu as pltpu
from jax.sharding import Mesh
from jax.sharding import PartitionSpec as P

HEAD = 64
FSDP = ("fsdp_0", "fsdp_1", "fsdp_2")
FSDP_REP = ("fsdp_0", "fsdp_1", "fsdp_2", "rep_0", "rep_1")

f32 = jnp.float32
bf16 = jnp.bfloat16

RING = 4


def place_of(y, z, x, c):
    return (((y % 2) * RING + z) * RING + x) * 4 + (y // 2) * 2 + c


def pairs(move):
    out = []
    for y in range(RING):
        for z in range(RING):
            for x in range(RING):
                for c in range(2):
                    ny, nz, nx, nc = move(y, z, x, c)
                    out.append((place_of(y, z, x, c), place_of(ny % RING, nz % RING, nx % RING, nc)))
    return out


def send(value, move):
    return lax.ppermute(value, FSDP_REP, pairs(move))


def along_y(step):
    return lambda y, z, x, c: (y + step, z, x, c)


def along_last(step):
    return lambda y, z, x, c: (y, z + step * c, x + step * (1 - c), c)


def along_mid(step):
    return lambda y, z, x, c: (y, z + step * (1 - c), x + step * c, c)


def to_partner(y, z, x, c):
    return (y, z, x, 1 - c)


MID = ((0, 0), (0, 1), (-1, 0), (-1, 1), (1, 0), (1, 1), (2, 0), (2, 1))
LAST = (0, -1, 1, 2)


def coordinates():
    return jnp.stack([lax.axis_index(name) for name in ("fsdp_1", "fsdp_2", "rep_1", "fsdp_0")]).astype(jnp.int32)


def block_row(where, block):
    z, x, c = where[0], where[1], where[2]
    last = LAST[block // 8]
    mid, half = MID[block % 8]
    zz = (z + mid * (1 - c) + last * c) & (RING - 1)
    xx = (x + last * (1 - c) + mid * c) & (RING - 1)
    return pl.multiple_of(half * 512 + zz * 128 + xx * 32, 32)


def in_vmem(n):
    return [pl.BlockSpec(memory_space=pltpu.VMEM)] * n


def in_smem():
    return pl.BlockSpec(memory_space=pltpu.SMEM)


def dot_nn(a, b):
    return lax.dot_general(a, b, (((1,), (0,)), ((), ())), preferred_element_type=f32)


def dot_nt(a, b):
    return lax.dot_general(a, b, (((1,), (1,)), ((), ())), preferred_element_type=f32)


def dot_tn(a, b):
    return lax.dot_general(a, b, (((0,), (0,)), ((), ())), preferred_element_type=f32)


def local_body(length, placed, where, own, peer, gain, *refs):
    size = own.shape[1]
    n_weights = 2 if placed else 20
    weights, refs = refs[:n_weights], refs[n_weights:]
    grads, refs = refs[:7], refs[7:]
    dh, gain_part, refs = refs[0], refs[1], refs[2:]
    if placed:
        before, weights = weights[1], weights[:1]
    hidden, hidden_t, dyb, qkv, datt, att, dqkv, gqkv, gout, wqkv, wout = refs

    if placed:
        (full,) = weights
        base = pl.multiple_of(where[2] * 512, 512)

        def w_qkv(n):
            top = pl.multiple_of((n // 5) * 1024, 1024)
            return full[pl.ds(top, 1024), pl.ds(pl.multiple_of((n % 5) * 256, 256), 256)]

        def w_out(half):
            return full[pl.ds(1024 + base, 512), 256 + 512 * half : 768 + 512 * half]
    else:
        for n, ref in enumerate(weights):
            for k in range(ref.shape[0]):
                at = block_row(where, PIECE_BLOCKS[n][k])
                wqkv[pl.ds(at, 32), :] = ref[k, :, :1536]
                wout[pl.ds(at, 32), :] = ref[k, :, 1536:]

        def w_qkv(n):
            return wqkv[:, pl.ds(pl.multiple_of(n * 256, 256), 256)]

        def w_out(half):
            return wout[512 * half : 512 * half + 512, :]

    for b, pair in enumerate((own, peer)):
        z = pair[0].astype(f32)
        inverse = lax.rsqrt(jnp.mean(z * z, axis=1, keepdims=True) + 1e-06)
        hidden[b * size : (b + 1) * size, :] = (z * inverse * gain[...]).astype(bf16)
        dyb[b * size : (b + 1) * size, :] = pair[1]
    hidden_t[...] = hidden[...].T

    @pl.loop(0, 6)
    def _(n):
        at = pl.multiple_of(n * 256, 256)
        qkv[:, pl.ds(at, 256)] = dot_nn(hidden[...], w_qkv(n)).astype(bf16)

    datt[...] = (dot_nt(dyb[:, :512], w_out(0)) + dot_nt(dyb[:, 512:], w_out(1))).astype(bf16)

    scale = HEAD ** (-0.5)
    lane = lax.broadcasted_iota(jnp.int32, (size, 128), 1)
    key_at = lax.broadcasted_iota(jnp.int32, (size, size), 1)
    zero = jnp.zeros((), bf16)

    @pl.loop(0, 8)
    def _(n):
        r = pl.ds(pl.multiple_of((n // 4) * size, 16), size)
        at = pl.multiple_of((n % 4) * 128, 128)
        query = qkv[r, pl.ds(at, 128)]
        keyed = qkv[r, pl.ds(at + 512, 128)]
        valued = qkv[r, pl.ds(at + 1024, 128)]
        dout = datt[r, pl.ds(at, 128)]
        sums = [None] * 4
        for head in range(2):
            mine = (lane < HEAD) if head == 0 else (lane >= HEAD)
            q = jnp.where(mine, query, zero)
            k = jnp.where(mine, keyed, zero)
            v = jnp.where(mine, valued, zero)
            d = jnp.where(mine, dout, zero)
            score = dot_nt(q, keyed) * scale
            score = jnp.where(key_at < length, score, -1e30)
            top = jnp.max(score, axis=1, keepdims=True)
            grown = jnp.exp(score - top)
            probs = grown * (1.0 / jnp.sum(grown, axis=1, keepdims=True))
            pb = probs.astype(bf16)
            dprob = dot_nt(d, valued)
            inner = jnp.sum(probs * dprob, axis=1, keepdims=True)
            dsb = (probs * (dprob - inner) * scale).astype(bf16)
            parts = (dot_nn(pb, v), dot_nn(dsb, k), dot_tn(dsb, q), dot_tn(pb, d))
            sums = [p if t is None else t + p for t, p in zip(sums, parts)]
        att[r, pl.ds(at, 128)] = sums[0].astype(bf16)
        dqkv[r, pl.ds(at, 128)] = sums[1].astype(bf16)
        dqkv[r, pl.ds(at + 512, 128)] = sums[2].astype(bf16)
        dqkv[r, pl.ds(at + 1024, 128)] = sums[3].astype(bf16)

    att_t = att[...].T
    for half in range(2):
        gout[512 * half : 512 * half + 512, :] = dot_nn(
            att_t, dyb[:, 512 * half : 512 * half + 512]
        ).astype(bf16)

    @pl.loop(0, 6)
    def _(n):
        at = pl.multiple_of(n * 256, 256)
        gqkv[:, pl.ds(at, 256)] = dot_nn(hidden_t[...], dqkv[:, pl.ds(at, 256)]).astype(bf16)

    for n, ref in enumerate(grads):
        for k, block in enumerate(GRAD_BLOCKS[n]):
            at = block_row(where, block)
            ref[32 * k : 32 * k + 32, :1536] = gqkv[pl.ds(at, 32), :]
            ref[32 * k : 32 * k + 32, 1536:] = gout[pl.ds(at, 32), :]

    part = jnp.zeros((1, 1024), f32)
    for b, pair in enumerate((own, peer)):
        total = dot_nt(dqkv[b * size : (b + 1) * size, :256], w_qkv(0))
        for k in range(1, 6):
            total = total + dot_nt(dqkv[b * size : (b + 1) * size, k * 256 : k * 256 + 256], w_qkv(k))
        dh[b] = total
        z = pair[0].astype(f32)
        normed = z * lax.rsqrt(jnp.mean(z * z, axis=1, keepdims=True) + 1e-06)
        part = part + jnp.sum(total * normed, axis=0, keepdims=True)
    if placed:
        both = jnp.concatenate([before[...], part], 1)
        gain_part[...] = both
        for ref in grads[5:]:
            ref[128:144, :] = in_pieces(both)
    else:
        gain_part[...] = part


def in_pieces(value):
    first = value.astype(bf16).astype(f32)
    second = (value - first).astype(bf16).astype(f32)
    third = value - first - second
    row = lax.broadcasted_iota(jnp.int32, (16, value.shape[1]), 0)
    out = jnp.where(row == 0, first, jnp.where(row == 1, second, third))
    return jnp.where(row < 3, out, 0.0).astype(bf16)


def from_pieces(rows):
    rows = rows.astype(f32)
    return (rows[0:1] + rows[1:2]) + rows[2:3]


PIECE_BLOCKS = []
for start in (0, 8, 16):
    PIECE_BLOCKS += [(start, start + 1), (start + 2, start + 3), (start + 4, start + 5), (start + 6,), (start + 7,)]
PIECE_BLOCKS += [(24, 25), (26, 27), (28, 29), (30,), (31,)]
GRAD_BLOCKS = [tuple(range(8))]
for start in (8, 16, 24):
    GRAD_BLOCKS += [tuple(range(start, start + 4)), tuple(range(start + 4, start + 8))]


def local_compute(length, placed, where, own, peer, gain, weights):
    size = own.shape[1]
    total = 2 * size
    return pl.pallas_call(
        lambda *refs: local_body(length, placed, *refs),
        in_specs=[in_smem()] + in_vmem(3 + len(weights)),
        out_specs=in_vmem(9),
        out_shape=[jax.ShapeDtypeStruct((256, 2048), bf16)]
        + [jax.ShapeDtypeStruct((128, 2048), bf16)] * 4
        + [jax.ShapeDtypeStruct((144 if placed else 128, 2048), bf16)] * 2
        + [
            jax.ShapeDtypeStruct((2, size, 1024), f32),
            jax.ShapeDtypeStruct((1, 2048 if placed else 1024), f32),
        ],
        scratch_shapes=[
            pltpu.VMEM((total, 1024), bf16),
            pltpu.VMEM((1024, total), bf16),
            pltpu.VMEM((total, 1024), bf16),
            pltpu.VMEM((total, 1536), bf16),
            pltpu.VMEM((total, 512), bf16),
            pltpu.VMEM((total, 512), bf16),
            pltpu.VMEM((total, 1536), bf16),
            pltpu.VMEM((1024, 1536), bf16),
            pltpu.VMEM((1024, 512), bf16),
            pltpu.VMEM((16 if placed else 1024, 1536), bf16),
            pltpu.VMEM((16 if placed else 1024, 512), bf16),
        ],
        name="local_placed" if placed else "local_pieces",
    )(where, own, peer, gain.reshape(1, 1024), *weights)


def my_columns(qkv_shard):
    c = lax.axis_index("rep_1")
    halves = qkv_shard.reshape(32, 3, 2, 512)
    return jnp.where(c == 0, halves[:, :, 0], halves[:, :, 1]).reshape(32, 1536)


def gather_by_calls(qkv_shard, out_shard):
    high = lax.axis_index("rep_0")
    shard = jnp.concatenate([my_columns(qkv_shard), out_shard], 1)
    shard = jnp.where(high == 0, shard[:, :1280], shard[:, 1280:])
    return lax.all_gather(shard, ("rep_0",) + FSDP, axis=0, tiled=True)


def gather_by_rings(qkv_shard, out_shard):
    low = lax.axis_index("fsdp_0")
    c = lax.axis_index("rep_1")
    shard = jnp.concatenate([my_columns(qkv_shard), out_shard], 1)
    top = send(shard[:16], along_y(1))
    bottom = send(shard[16:], along_y(-1))
    other = jnp.concatenate([top, bottom], 0)
    first = jnp.where(low == 0, shard[:, :1536], other[:, :1536])
    second = jnp.where(low == 0, other[:, :1536], shard[:, :1536])
    outw = jnp.where(low == c, shard[:, 1536:], other[:, 1536:])
    block = jnp.stack(
        [
            jnp.concatenate([first, outw[:, :512]], 1),
            jnp.concatenate([second, outw[:, 512:]], 1),
        ]
    )
    left = send(block, along_mid(1))
    right = send(block, along_mid(-1))
    far_a = send(left[:1], along_mid(1))
    far_b = send(right[1:], along_mid(-1))
    own = [block, left, right, far_a, far_b]
    from_left = [send(piece, along_last(1)) for piece in own]
    from_right = [send(piece, along_last(-1)) for piece in own]
    across = [send(piece, along_last(1)) for piece in from_left[:2]]
    across += [send(piece, along_last(-1)) for piece in from_right[2:]]
    return own + from_left + from_right + across


def add(*terms):
    total = terms[0].astype(f32)
    for term in terms[1:]:
        total = total + term.astype(f32)
    return total


def in_one_kernel(body, shapes, *args, scalars=None):
    specs = in_vmem(len(args))
    if scalars is not None:
        specs = [in_smem()] + specs
        args = (scalars,) + args
    return pl.pallas_call(
        body,
        in_specs=specs,
        out_specs=in_vmem(len(shapes)),
        out_shape=[jax.ShapeDtypeStruct(shape, dtype) for shape, dtype in shapes],
    )(*args)


def fold_far(right, left, up, down, right_out, left_out):
    right_out[:128, :] = add(right[...], up[:128, :]).astype(bf16)
    left_out[...] = add(left[...], down[:128, :]).astype(bf16)
    if right_out.shape[0] > 128:
        right_out[128:, :] = up[128:, :]


def first_steps(grads):
    own, left_a, left_b, right_a, right_b, far_a, far_b = grads
    up_far = send(far_a, along_last(1))
    down_far = send(far_b, along_last(-1))
    up_b = send(right_b, along_last(1))
    down_a = send(left_a, along_last(-1))
    return own, left_b, right_a, up_far, down_far, up_b, down_a


def second_steps(parts):
    own, left_b, right_a, up_far, down_far, up_b, down_a = parts
    right, left = in_one_kernel(
        fold_far, [(up_far.shape, bf16), ((128, 2048), bf16)], right_a, left_b, up_far, down_far
    )
    up_a = send(right, along_last(1))
    down_b = send(left, along_last(-1))
    return own, up_a, up_b, down_a, down_b


def ring_sum(own, left, right, far):
    return (own + far) + (left + right)


def fold_last(v_own, v_up_a, v_up_b, v_down_a, v_down_b, own, up_a, up_b, down_a, down_b,
              gain, up_far, down_far, far_up, far_down, right, left, home, gain_out):
    parts = (
        (v_own, v_up_a, v_up_b, v_down_a, v_down_b),
        (own, up_a, up_b, down_a, down_b),
    )
    for s, (o, ua, ub, da, db) in enumerate(parts):
        for j in range(8):
            u, d, at = (ua, da, 32 * j) if j < 4 else (ub, db, 32 * j - 128)
            total = add(o[32 * j : 32 * j + 32, :], u[at : at + 32, :], d[at : at + 32, :])
            if j < 2:
                home[64 * s + 32 * j : 64 * s + 32 * j + 32, :] = total
            else:
                ref = (left, right, None)[(j - 2) // 2]
                if ref is None:
                    ref = far_up if j == 6 else far_down
                    ref[32 * s : 32 * s + 32, :] = total.astype(bf16)
                else:
                    row = 64 * s + 32 * (j % 2)
                    ref[row : row + 32, :] = total.astype(bf16)
    total = ring_sum(
        gain[...],
        from_pieces(up_far[128:144, :]),
        from_pieces(down_far[128:144, :]),
        from_pieces(up_a[128:144, :]),
    )
    gain_out[...] = total
    far_up[64:80, :] = in_pieces(total)
    far_down[64:80, :] = in_pieces(total)


def fold_mid_far(right, left, up, down, right_out, left_out):
    for s in range(2):
        a, b, c = 64 * s, 64 * s + 32, 64 * s + 64
        right_out[a:b, :] = add(right[a:b, :], up[32 * s : 32 * s + 32, :]).astype(bf16)
        right_out[b:c, :] = right[b:c, :]
        left_out[a:b, :] = left[a:b, :]
        left_out[b:c, :] = add(left[b:c, :], down[32 * s : 32 * s + 32, :]).astype(bf16)
    right_out[128:144, :] = up[64:80, :]


def fold_mid(where, home, gain, up, down, up_far, down_far, same, cross, gain_out):
    low = where[3]
    for s in range(2):
        first, second = (
            add(home[r, :], up[r, :], down[r, :]).astype(bf16)
            for r in (pl.ds(64 * s, 32), pl.ds(64 * s + 32, 32))
        )
        r = slice(32 * s, 32 * s + 32)
        flip = jnp.full((32, 1536), low, jnp.int32) == 1
        a, b = first[:, :1536].astype(f32), second[:, :1536].astype(f32)
        same[r, :1536] = jnp.where(flip, b, a).astype(bf16)
        cross[r, :1536] = jnp.where(flip, a, b).astype(bf16)
        for ref in (same, cross):
            ref[r, 1536:2048] = first[:, 1536:]
            ref[r, 2048:] = second[:, 1536:]
    total = ring_sum(
        gain[...],
        from_pieces(up_far[64:80, :]),
        from_pieces(down_far[64:80, :]),
        from_pieces(up[128:144, :]),
    )
    gain_out[...] = total
    for ref in (same, cross):
        ref[64:80, :2048] = in_pieces(total)
        ref[64:80, 2048:] = jnp.zeros((16, 512), bf16)


def fold_y(count, same, up, down, far, gain, out):
    total = add(same[:64, :], far[:64, :]) + add(up[:64, :], down[:64, :])
    out[:64, :] = total / count
    total = ring_sum(
        gain[...],
        from_pieces(up[64:80, :2048]),
        from_pieces(down[64:80, :2048]),
        from_pieces(far[64:80, :2048]),
    )
    out[64:72, :2048] = jnp.broadcast_to(total, (8, 2048))
    out[64:72, 2048:] = jnp.zeros((8, 512), f32)


def spread(count, where, mine, peer, v_qkv, v_out, a_qkv, a_out, gain_v, gain_a):
    c, low = where[2], where[3]
    for s, (qkv, out) in enumerate(((v_qkv, v_out), (a_qkv, a_out))):
        r = slice(32 * s, 32 * s + 32)
        for k in range(3):
            at = pl.multiple_of(1024 * k + 512 * c, 512)
            qkv[:, pl.ds(at, 512)] = mine[r, 512 * k : 512 * k + 512]
            at = pl.multiple_of(1024 * k + 512 * (1 - c), 512)
            qkv[:, pl.ds(at, 512)] = peer[r, 512 * k : 512 * k + 512]
        here = jnp.full((32, 1024), (low == c).astype(jnp.int32), jnp.int32) == 1
        out[...] = jnp.where(here, mine[r, 1536:], peer[r, 1536:])
    total = (mine[64:72, :2048] + peer[64:72, :2048]) / count
    gain_v[...] = total[0:1, :1024]
    gain_a[...] = total[0:1, 1024:]


def last_steps(video, audio, audio_parts, gain, where, count):
    audio_far = audio_parts[3:5]
    far_up, far_down, right, left, home, gain = in_one_kernel(
        fold_last,
        [((80, 2048), bf16)] * 2
        + [((128, 2048), bf16)] * 2
        + [((128, 2048), f32), ((1, 2048), f32)],
        *video,
        *audio,
        gain,
        *audio_far,
    )
    up_far = send(far_up, along_mid(1))
    down_far = send(far_down, along_mid(-1))
    right, left = in_one_kernel(
        fold_mid_far, [((144, 2048), bf16), ((128, 2048), bf16)], right, left, up_far, down_far
    )
    up = send(right, along_mid(1))
    down = send(left, along_mid(-1))
    same, cross, gain = in_one_kernel(
        fold_mid,
        [((80, 2560), bf16)] * 2 + [((1, 2048), f32)],
        home,
        gain,
        up,
        down,
        up_far,
        down_far,
        scalars=where,
    )
    far = send(same, along_y(2))
    up = send(cross, along_y(1))
    down = send(cross, along_y(-1))
    (total,) = in_one_kernel(
        functools.partial(fold_y, count), [((72, 2560), f32)], same, up, down, far, gain
    )
    peer = send(total, to_partner)
    return in_one_kernel(
        functools.partial(spread, count),
        [((32, 3072), f32), ((32, 1024), f32)] * 2 + [((1, 1024), f32)] * 2,
        total,
        peer,
        scalars=where,
    )


def clip_pair(tokens, bottle, d_tokens, d_bottle):
    half = (d_bottle.astype(f32) * 0.5).astype(bf16)
    pad = jnp.zeros((-(tokens.shape[0] + bottle.shape[0]) % 16, 1024), bf16)
    own = jnp.stack(
        [jnp.concatenate([tokens, bottle, pad], 0), jnp.concatenate([d_tokens, half, pad], 0)]
    )
    return own, send(own, to_partner)


def finish(own, gain, dh):
    dhidden = dh[0] + send(dh[1], to_partner)
    z = own[0].astype(f32)
    inverse = lax.rsqrt(jnp.mean(z * z, axis=1, keepdims=True) + 1e-06)
    normed = z * inverse
    dnorm = dhidden * gain
    d_out = own[1].astype(f32)
    d_z = d_out + inverse * (dnorm - normed * jnp.mean(dnorm * normed, axis=1, keepdims=True))
    return d_z


def per_device(
    video_in,
    audio_in,
    bottle_in,
    video_gain,
    audio_gain,
    video_qkv,
    video_out,
    audio_qkv,
    audio_out,
    grad_video,
    grad_audio,
    grad_bottle,
):
    count = float(video_in.shape[0] * lax.axis_size(FSDP_REP))
    where = coordinates()
    video_len = video_in.shape[1]
    audio_len = audio_in.shape[1]
    bottle_len = bottle_in.shape[1]
    aweights = gather_by_calls(audio_qkv, audio_out)
    vweights = gather_by_rings(video_qkv, video_out)
    vown, vpeer = clip_pair(video_in[0], bottle_in[0], grad_video[0], grad_bottle[0])
    aown, apeer = clip_pair(audio_in[0], bottle_in[0], grad_audio[0], grad_bottle[0])
    vpeer, apeer = lax.optimization_barrier((vpeer, apeer))
    *grads, dh_video, gain_v = local_compute(
        video_len + bottle_len, False, where, vown, vpeer, video_gain, vweights
    )
    video_parts = first_steps(grads)
    *grads, dh_audio, gain = local_compute(
        audio_len + bottle_len,
        True,
        where,
        aown,
        apeer,
        audio_gain,
        [aweights, gain_v],
    )
    audio_parts = first_steps(grads)
    video = second_steps(video_parts)
    audio = second_steps(audio_parts)
    (
        video_qkv_grad,
        video_out_grad,
        audio_qkv_grad,
        audio_out_grad,
        gain_v,
        gain_a,
    ) = last_steps(video, audio, audio_parts, gain, where, count)
    dz_video = finish(vown, video_gain, dh_video)
    dz_audio = finish(aown, audio_gain, dh_audio)
    video_end = video_len + bottle_len
    audio_end = audio_len + bottle_len
    dvideo_in = dz_video[None, :video_len].astype(bf16)
    daudio_in = dz_audio[None, :audio_len].astype(bf16)
    dbottle_in = dz_video[None, video_len:video_end] + dz_audio[None, audio_len:audio_end]
    dbottle_in = dbottle_in.astype(bf16)
    return (
        dvideo_in,
        daudio_in,
        dbottle_in,
        video_qkv_grad,
        video_out_grad,
        audio_qkv_grad,
        audio_out_grad,
        gain_v[0],
        gain_a[0],
    )


def solution(mesh):
    split = Mesh(
        mesh.devices.reshape(2, 4, 4, 2, 2), ("fsdp_0", "fsdp_1", "fsdp_2", "rep_0", "rep_1")
    )
    return jax.shard_map(
        per_device,
        mesh=split,
        in_specs=(
            P(FSDP_REP, None, None),
            P(FSDP_REP, None, None),
            P(FSDP_REP, None, None),
            P(),
            P(),
            P(FSDP, None),
            P(FSDP, None),
            P(FSDP, None),
            P(FSDP, None),
            P(FSDP_REP, None, None),
            P(FSDP_REP, None, None),
            P(FSDP_REP, None, None),
        ),
        out_specs=(
            P(FSDP_REP, None, None),
            P(FSDP_REP, None, None),
            P(FSDP_REP, None, None),
            P(FSDP, None),
            P(FSDP, None),
            P(FSDP, None),
            P(FSDP, None),
            P(),
            P(),
        ),
        check_vma=False,
    )
```

```python
import functools

import jax
import jax.numpy as jnp
from jax import lax
from jax.experimental import pallas as pl
from jax.experimental.pallas import tpu as pltpu
from jax.sharding import Mesh
from jax.sharding import PartitionSpec as P

HEAD = 64
FSDP = ("fsdp_0", "fsdp_1", "fsdp_2")
FSDP_REP = ("fsdp_0", "fsdp_1", "fsdp_2", "rep_0", "rep_1")

f32 = jnp.float32
bf16 = jnp.bfloat16

RING = 4


def place_of(y, z, x, c):
    return (((y % 2) * RING + z) * RING + x) * 4 + (y // 2) * 2 + c


def pairs(move):
    out = []
    for y in range(RING):
        for z in range(RING):
            for x in range(RING):
                for c in range(2):
                    ny, nz, nx, nc = move(y, z, x, c)
                    out.append((place_of(y, z, x, c), place_of(ny % RING, nz % RING, nx % RING, nc)))
    return out


def send(value, move):
    return lax.ppermute(value, FSDP_REP, pairs(move))


def along_y(step):
    return lambda y, z, x, c: (y + step, z, x, c)


def along_last(step):
    return lambda y, z, x, c: (y, z + step * c, x + step * (1 - c), c)


def along_mid(step):
    return lambda y, z, x, c: (y, z + step * (1 - c), x + step * c, c)


def to_partner(y, z, x, c):
    return (y, z, x, 1 - c)


MID = ((0, 0), (0, 1), (-1, 0), (-1, 1), (1, 0), (1, 1), (2, 0), (2, 1))
LAST = (0, -1, 1, 2)


def coordinates():
    return jnp.stack([lax.axis_index(name) for name in ("fsdp_1", "fsdp_2", "rep_1", "fsdp_0")]).astype(jnp.int32)


def block_row(where, block):
    z, x, c = where[0], where[1], where[2]
    last = LAST[block // 8]
    mid, half = MID[block % 8]
    zz = (z + mid * (1 - c) + last * c) & (RING - 1)
    xx = (x + last * (1 - c) + mid * c) & (RING - 1)
    return pl.multiple_of(half * 512 + zz * 128 + xx * 32, 32)


def in_vmem(n):
    return [pl.BlockSpec(memory_space=pltpu.VMEM)] * n


def in_smem():
    return pl.BlockSpec(memory_space=pltpu.SMEM)


def dot_nn(a, b):
    return lax.dot_general(a, b, (((1,), (0,)), ((), ())), preferred_element_type=f32)


def dot_nt(a, b):
    return lax.dot_general(a, b, (((1,), (1,)), ((), ())), preferred_element_type=f32)


def dot_tn(a, b):
    return lax.dot_general(a, b, (((0,), (0,)), ((), ())), preferred_element_type=f32)


def local_body(length, placed, where, own, peer, gain, *refs):
    size = own.shape[1]
    n_weights = 2 if placed else 20
    weights, refs = refs[:n_weights], refs[n_weights:]
    grads, refs = refs[:7], refs[7:]
    dh, gain_part, refs = refs[:2], refs[2], refs[3:]
    if placed:
        before, weights = weights[1], weights[:1]
    hidden, hidden_t, dyb, qkv, datt, att, dqkv, gqkv, gout, wqkv, wout = refs

    if placed:
        (full,) = weights
        base = pl.multiple_of(where[2] * 512, 512)

        def w_qkv(n):
            top = pl.multiple_of((n // 5) * 1024, 1024)
            return full[pl.ds(top, 1024), pl.ds(pl.multiple_of((n % 5) * 256, 256), 256)]

        def w_out(half):
            return full[pl.ds(1024 + base, 512), 256 + 512 * half : 768 + 512 * half]
    else:
        for n, ref in enumerate(weights):
            for k in range(ref.shape[0]):
                at = block_row(where, PIECE_BLOCKS[n][k])
                wqkv[pl.ds(at, 32), :] = ref[k, :, :1536]
                wout[pl.ds(at, 32), :] = ref[k, :, 1536:]

        def w_qkv(n):
            return wqkv[:, pl.ds(pl.multiple_of(n * 256, 256), 256)]

        def w_out(half):
            return wout[512 * half : 512 * half + 512, :]

    for b, pair in enumerate((own, peer)):
        z = pair[0].astype(f32)
        inverse = lax.rsqrt(jnp.mean(z * z, axis=1, keepdims=True) + 1e-06)
        hidden[b * size : (b + 1) * size, :] = (z * inverse * gain[...]).astype(bf16)
        dyb[b * size : (b + 1) * size, :] = pair[1]
    hidden_t[...] = hidden[...].T

    for n in range(6):
        qkv[:, 256 * n : 256 * n + 256] = dot_nn(hidden[...], w_qkv(n)).astype(bf16)

    datt[...] = (dot_nt(dyb[:, :512], w_out(0)) + dot_nt(dyb[:, 512:], w_out(1))).astype(bf16)

    scale = jnp.asarray(HEAD ** (-0.5), bf16)
    lane = lax.broadcasted_iota(jnp.int32, (size, 128), 1)
    key_at = lax.broadcasted_iota(jnp.int32, (size, size), 1)
    zero = jnp.zeros((), bf16)

    @pl.loop(0, 8, unroll=2)
    def _(n):
        r = pl.ds(pl.multiple_of((n // 4) * size, 16), size)
        at = pl.multiple_of((n % 4) * 128, 128)
        query = qkv[r, pl.ds(at, 128)]
        keyed = qkv[r, pl.ds(at + 512, 128)]
        valued = qkv[r, pl.ds(at + 1024, 128)]
        dout = datt[r, pl.ds(at, 128)]
        sums = [None] * 4
        for head in range(2):
            mine = (lane < HEAD) if head == 0 else (lane >= HEAD)
            q = jnp.where(mine, query * scale, zero)
            k = jnp.where(mine, keyed * scale, zero)
            v = jnp.where(mine, valued, zero)
            d = jnp.where(mine, dout, zero)
            score = dot_nt(q, keyed)
            score = jnp.where(key_at < length, score, -1e30)
            top = jnp.max(score, axis=1, keepdims=True)
            grown = jnp.exp(score - top)
            probs = grown * (1.0 / jnp.sum(grown, axis=1, keepdims=True))
            pb = probs.astype(bf16)
            dprob = dot_nt(d, valued)
            inner = jnp.sum(probs * dprob, axis=1, keepdims=True)
            dsb = (probs * (dprob - inner)).astype(bf16)
            parts = (dot_nn(pb, v), dot_nn(dsb, k), dot_tn(dsb, q), dot_tn(pb, d))
            sums = [p if t is None else t + p for t, p in zip(sums, parts)]
        att[r, pl.ds(at, 128)] = sums[0].astype(bf16)
        dqkv[r, pl.ds(at, 128)] = sums[1].astype(bf16)
        dqkv[r, pl.ds(at + 512, 128)] = sums[2].astype(bf16)
        dqkv[r, pl.ds(at + 1024, 128)] = sums[3].astype(bf16)

    att_t = att[...].T
    for half in range(2):
        gout[512 * half : 512 * half + 512, :] = dot_nn(
            att_t, dyb[:, 512 * half : 512 * half + 512]
        ).astype(bf16)

    gqkv[...] = dot_nn(hidden_t[...], dqkv[...]).astype(bf16)

    for n, ref in enumerate(grads):
        for k, block in enumerate(GRAD_BLOCKS[n]):
            at = block_row(where, block)
            ref[32 * k : 32 * k + 32, :1536] = gqkv[pl.ds(at, 32), :]
            ref[32 * k : 32 * k + 32, 1536:] = gout[pl.ds(at, 32), :]

    part = jnp.zeros((1, 1024), f32)
    for b, pair in enumerate((own, peer)):
        total = dot_nt(dqkv[b * size : (b + 1) * size, :256], w_qkv(0))
        for k in range(1, 6):
            total = total + dot_nt(dqkv[b * size : (b + 1) * size, k * 256 : k * 256 + 256], w_qkv(k))
        dh[b][...] = total
        z = pair[0].astype(f32)
        normed = z * lax.rsqrt(jnp.mean(z * z, axis=1, keepdims=True) + 1e-06)
        part = part + jnp.sum(total * normed, axis=0, keepdims=True)
    if placed:
        both = jnp.concatenate([before[...], part], 1)
        gain_part[...] = both
        for ref in grads[5:]:
            ref[128:144, :] = in_pieces(both)
    else:
        gain_part[...] = part


def in_pieces(value):
    first = value.astype(bf16).astype(f32)
    second = (value - first).astype(bf16).astype(f32)
    third = value - first - second
    row = lax.broadcasted_iota(jnp.int32, (16, value.shape[1]), 0)
    out = jnp.where(row == 0, first, jnp.where(row == 1, second, third))
    return jnp.where(row < 3, out, 0.0).astype(bf16)


def from_pieces(rows):
    rows = rows.astype(f32)
    return (rows[0:1] + rows[1:2]) + rows[2:3]


PIECE_BLOCKS = []
for start in (0, 8, 16):
    PIECE_BLOCKS += [(start, start + 1), (start + 2, start + 3), (start + 4, start + 5), (start + 6,), (start + 7,)]
PIECE_BLOCKS += [(24, 25), (26, 27), (28, 29), (30,), (31,)]
GRAD_BLOCKS = [tuple(range(8))]
for start in (8, 16, 24):
    GRAD_BLOCKS += [tuple(range(start, start + 4)), tuple(range(start + 4, start + 8))]


def local_compute(length, placed, where, own, peer, gain, weights):
    size = own.shape[1]
    total = 2 * size
    return pl.pallas_call(
        lambda *refs: local_body(length, placed, *refs),
        in_specs=[in_smem()] + in_vmem(3 + len(weights)),
        out_specs=in_vmem(10),
        out_shape=[jax.ShapeDtypeStruct((256, 2048), bf16)]
        + [jax.ShapeDtypeStruct((128, 2048), bf16)] * 4
        + [jax.ShapeDtypeStruct((144 if placed else 128, 2048), bf16)] * 2
        + [
            jax.ShapeDtypeStruct((size, 1024), f32),
            jax.ShapeDtypeStruct((size, 1024), f32),
            jax.ShapeDtypeStruct((1, 2048 if placed else 1024), f32),
        ],
        scratch_shapes=[
            pltpu.VMEM((total, 1024), bf16),
            pltpu.VMEM((1024, total), bf16),
            pltpu.VMEM((total, 1024), bf16),
            pltpu.VMEM((total, 1536), bf16),
            pltpu.VMEM((total, 512), bf16),
            pltpu.VMEM((total, 512), bf16),
            pltpu.VMEM((total, 1536), bf16),
            pltpu.VMEM((1024, 1536), bf16),
            pltpu.VMEM((1024, 512), bf16),
            pltpu.VMEM((16 if placed else 1024, 1536), bf16),
            pltpu.VMEM((16 if placed else 1024, 512), bf16),
        ],
        name="local_placed" if placed else "local_pieces",
    )(where, own, peer, gain.reshape(1, 1024), *weights)


def my_columns(qkv_shard):
    c = lax.axis_index("rep_1")
    halves = qkv_shard.reshape(32, 3, 2, 512)
    return jnp.where(c == 0, halves[:, :, 0], halves[:, :, 1]).reshape(32, 1536)


def gather_by_calls(qkv_shard, out_shard):
    high = lax.axis_index("rep_0")
    shard = jnp.concatenate([my_columns(qkv_shard), out_shard], 1)
    shard = jnp.where(high == 0, shard[:, :1280], shard[:, 1280:])
    return lax.all_gather(shard, ("rep_0",) + FSDP, axis=0, tiled=True)


def gather_by_rings(qkv_shard, out_shard):
    low = lax.axis_index("fsdp_0")
    c = lax.axis_index("rep_1")
    shard = jnp.concatenate([my_columns(qkv_shard), out_shard], 1)
    top = send(shard[:16], along_y(1))
    bottom = send(shard[16:], along_y(-1))
    other = jnp.concatenate([top, bottom], 0)
    first = jnp.where(low == 0, shard[:, :1536], other[:, :1536])
    second = jnp.where(low == 0, other[:, :1536], shard[:, :1536])
    outw = jnp.where(low == c, shard[:, 1536:], other[:, 1536:])
    block = jnp.stack(
        [
            jnp.concatenate([first, outw[:, :512]], 1),
            jnp.concatenate([second, outw[:, 512:]], 1),
        ]
    )
    left = send(block, along_mid(1))
    right = send(block, along_mid(-1))
    far_a = send(left[:1], along_mid(1))
    far_b = send(right[1:], along_mid(-1))
    own = [block, left, right, far_a, far_b]
    from_left = [send(piece, along_last(1)) for piece in own]
    from_right = [send(piece, along_last(-1)) for piece in own]
    across = [send(piece, along_last(1)) for piece in from_left[:2]]
    across += [send(piece, along_last(-1)) for piece in from_right[2:]]
    return own + from_left + from_right + across


def add(*terms):
    total = terms[0].astype(f32)
    for term in terms[1:]:
        total = total + term.astype(f32)
    return total


def in_one_kernel(body, shapes, *args, scalars=None):
    specs = in_vmem(len(args))
    if scalars is not None:
        specs = [in_smem()] + specs
        args = (scalars,) + args
    return pl.pallas_call(
        body,
        in_specs=specs,
        out_specs=in_vmem(len(shapes)),
        out_shape=[jax.ShapeDtypeStruct(shape, dtype) for shape, dtype in shapes],
    )(*args)


def fold_far(right, left, up, down, right_out, left_out):
    right_out[:128, :] = add(right[...], up[:128, :]).astype(bf16)
    left_out[...] = add(left[...], down[:128, :]).astype(bf16)
    if right_out.shape[0] > 128:
        right_out[128:, :] = up[128:, :]


def first_steps(grads):
    own, left_a, left_b, right_a, right_b, far_a, far_b = grads
    up_far = send(far_a, along_last(1))
    down_far = send(far_b, along_last(-1))
    up_b = send(right_b, along_last(1))
    down_a = send(left_a, along_last(-1))
    return own, left_b, right_a, up_far, down_far, up_b, down_a


def second_steps(parts):
    own, left_b, right_a, up_far, down_far, up_b, down_a = parts
    right, left = in_one_kernel(
        fold_far, [(up_far.shape, bf16), ((128, 2048), bf16)], right_a, left_b, up_far, down_far
    )
    up_a = send(right, along_last(1))
    down_b = send(left, along_last(-1))
    return own, up_a, up_b, down_a, down_b


def ring_sum(own, left, right, far):
    return (own + far) + (left + right)


def fold_sum(own, up_a, up_b, down_a, down_b, out):
    out[:128, :] = add(own[:128, :], up_a[:128, :], down_a[:128, :]).astype(bf16)
    out[128:, :] = add(own[128:, :], up_b[...], down_b[...]).astype(bf16)


def fold_last(video, own, up_a, up_b, down_a, down_b, gain, up_far, down_far,
              far_up, far_down, right, left, home, gain_out):
    for s in range(2):
        for j in range(8):
            u, d, at = (up_a, down_a, 32 * j) if j < 4 else (up_b, down_b, 32 * j - 128)
            if s == 0:
                total = video[32 * j : 32 * j + 32, :].astype(f32)
            else:
                total = add(own[32 * j : 32 * j + 32, :], u[at : at + 32, :], d[at : at + 32, :])
            if j < 2:
                home[64 * s + 32 * j : 64 * s + 32 * j + 32, :] = total
            elif j < 6:
                row = 64 * s + 32 * (j % 2)
                (left if j < 4 else right)[row : row + 32, :] = total.astype(bf16)
            else:
                (far_up if j == 6 else far_down)[32 * s : 32 * s + 32, :] = total.astype(bf16)
    total = ring_sum(
        gain[...],
        from_pieces(up_far[128:144, :]),
        from_pieces(down_far[128:144, :]),
        from_pieces(up_a[128:144, :]),
    )
    gain_out[...] = total
    far_up[64:80, :] = in_pieces(total)
    far_down[64:80, :] = in_pieces(total)


def fold_mid_far(right, left, up, down, right_out, left_out):
    for s in range(2):
        a, b, c = 64 * s, 64 * s + 32, 64 * s + 64
        right_out[a:b, :] = add(right[a:b, :], up[32 * s : 32 * s + 32, :]).astype(bf16)
        right_out[b:c, :] = right[b:c, :]
        left_out[a:b, :] = left[a:b, :]
        left_out[b:c, :] = add(left[b:c, :], down[32 * s : 32 * s + 32, :]).astype(bf16)
    right_out[128:144, :] = up[64:80, :]


def fold_mid(where, home, gain, up, down, up_far, down_far, same, cross, gain_out):
    low = where[3]
    for s in range(2):
        first, second = (
            add(home[r, :], up[r, :], down[r, :]).astype(bf16)
            for r in (pl.ds(64 * s, 32), pl.ds(64 * s + 32, 32))
        )
        r = slice(32 * s, 32 * s + 32)
        flip = jnp.full((32, 1536), low, jnp.int32) == 1
        a, b = first[:, :1536].astype(f32), second[:, :1536].astype(f32)
        same[r, :1536] = jnp.where(flip, b, a).astype(bf16)
        cross[r, :1536] = jnp.where(flip, a, b).astype(bf16)
        for ref in (same, cross):
            ref[r, 1536:2048] = first[:, 1536:]
            ref[r, 2048:] = second[:, 1536:]
    total = ring_sum(
        gain[...],
        from_pieces(up_far[64:80, :]),
        from_pieces(down_far[64:80, :]),
        from_pieces(up[128:144, :]),
    )
    gain_out[...] = total
    for ref in (same, cross):
        ref[64:72, :2048] = in_pieces(total)[:8]
        ref[64:72, 2048:] = jnp.zeros((8, 512), bf16)


def fold_y(count, same, up, down, far, gain, out):
    total = add(same[:64, :], far[:64, :]) + add(up[:64, :], down[:64, :])
    out[:64, :] = total / count
    total = ring_sum(
        gain[...],
        from_pieces(up[64:72, :2048]),
        from_pieces(down[64:72, :2048]),
        from_pieces(far[64:72, :2048]),
    )
    out[64:72, :2048] = jnp.broadcast_to(total, (8, 2048))
    out[64:72, 2048:] = jnp.zeros((8, 512), f32)


def spread(count, where, mine, peer, v_qkv, v_out, a_qkv, a_out, gain_v, gain_a):
    c, low = where[2], where[3]
    for s, (qkv, out) in enumerate(((v_qkv, v_out), (a_qkv, a_out))):
        r = slice(32 * s, 32 * s + 32)
        for k in range(3):
            at = pl.multiple_of(1024 * k + 512 * c, 512)
            qkv[:, pl.ds(at, 512)] = mine[r, 512 * k : 512 * k + 512]
            at = pl.multiple_of(1024 * k + 512 * (1 - c), 512)
            qkv[:, pl.ds(at, 512)] = peer[r, 512 * k : 512 * k + 512]
        here = jnp.full((32, 1024), (low == c).astype(jnp.int32), jnp.int32) == 1
        out[...] = jnp.where(here, mine[r, 1536:], peer[r, 1536:])
    total = (mine[64:72, :2048] + peer[64:72, :2048]) / count
    gain_v[...] = total[0:1, :1024]
    gain_a[...] = total[0:1, 1024:]


def last_steps(video, audio, audio_parts, gain, where, count):
    audio_far = audio_parts[3:5]
    (video_sum,) = in_one_kernel(fold_sum, [((256, 2048), bf16)], *video)
    far_up, far_down, right, left, home, gain = in_one_kernel(
        fold_last,
        [((80, 2048), bf16)] * 2
        + [((128, 2048), bf16)] * 2
        + [((128, 2048), f32), ((1, 2048), f32)],
        video_sum,
        *audio,
        gain,
        *audio_far,
    )
    up_far = send(far_up, along_mid(1))
    down_far = send(far_down, along_mid(-1))
    right, left = in_one_kernel(
        fold_mid_far, [((144, 2048), bf16), ((128, 2048), bf16)], right, left, up_far, down_far
    )
    up = send(right, along_mid(1))
    down = send(left, along_mid(-1))
    same, cross, gain = in_one_kernel(
        fold_mid,
        [((72, 2560), bf16)] * 2 + [((1, 2048), f32)],
        home,
        gain,
        up,
        down,
        up_far,
        down_far,
        scalars=where,
    )
    far = send(same, along_y(2))
    up = send(cross, along_y(1))
    down = send(cross, along_y(-1))
    (total,) = in_one_kernel(
        functools.partial(fold_y, count), [((72, 2560), f32)], same, up, down, far, gain
    )
    peer = send(total, to_partner)
    return in_one_kernel(
        functools.partial(spread, count),
        [((32, 3072), f32), ((32, 1024), f32)] * 2 + [((1, 1024), f32)] * 2,
        total,
        peer,
        scalars=where,
    )


def clip_pair(tokens, bottle, d_tokens, d_bottle):
    half = (d_bottle.astype(f32) * 0.5).astype(bf16)
    pad = jnp.zeros((-(tokens.shape[0] + bottle.shape[0]) % 16, 1024), bf16)
    own = jnp.stack(
        [jnp.concatenate([tokens, bottle, pad], 0), jnp.concatenate([d_tokens, half, pad], 0)]
    )
    return own, send(own, to_partner)


def finish(own, gain, dh, dh_peer):
    from_peer = send(dh_peer, to_partner)
    dhidden = dh + from_peer
    z = own[0].astype(f32)
    inverse = lax.rsqrt(jnp.mean(z * z, axis=1, keepdims=True) + 1e-06)
    normed = z * inverse
    dnorm = dhidden * gain
    d_out = own[1].astype(f32)
    mean = jnp.mean(dnorm * normed, axis=1, keepdims=True)
    return d_out + inverse * (dnorm - normed * mean)


def per_device(
    video_in,
    audio_in,
    bottle_in,
    video_gain,
    audio_gain,
    video_qkv,
    video_out,
    audio_qkv,
    audio_out,
    grad_video,
    grad_audio,
    grad_bottle,
):
    count = float(video_in.shape[0] * lax.axis_size(FSDP_REP))
    where = coordinates()
    video_len = video_in.shape[1]
    audio_len = audio_in.shape[1]
    bottle_len = bottle_in.shape[1]
    aweights = gather_by_calls(audio_qkv, audio_out)
    vweights = gather_by_rings(video_qkv, video_out)
    vown, vpeer = clip_pair(video_in[0], bottle_in[0], grad_video[0], grad_bottle[0])
    aown, apeer = clip_pair(audio_in[0], bottle_in[0], grad_audio[0], grad_bottle[0])
    vpeer, apeer = lax.optimization_barrier((vpeer, apeer))
    *grads, dh_video, dh_video_peer, gain_v = local_compute(
        video_len + bottle_len, False, where, vown, vpeer, video_gain, vweights
    )
    video_parts = first_steps(grads)
    *grads, dh_audio, dh_audio_peer, gain = local_compute(
        audio_len + bottle_len,
        True,
        where,
        aown,
        apeer,
        audio_gain,
        [aweights, gain_v],
    )
    audio_parts = first_steps(grads)
    video = second_steps(video_parts)
    audio = second_steps(audio_parts)
    (
        video_qkv_grad,
        video_out_grad,
        audio_qkv_grad,
        audio_out_grad,
        gain_v,
        gain_a,
    ) = last_steps(video, audio, audio_parts, gain, where, count)
    dz_video = finish(vown, video_gain, dh_video, dh_video_peer)
    dz_audio = finish(aown, audio_gain, dh_audio, dh_audio_peer)
    video_end = video_len + bottle_len
    audio_end = audio_len + bottle_len
    dvideo_in = dz_video[None, :video_len].astype(bf16)
    daudio_in = dz_audio[None, :audio_len].astype(bf16)
    dbottle_in = dz_video[None, video_len:video_end] + dz_audio[None, audio_len:audio_end]
    dbottle_in = dbottle_in.astype(bf16)
    return (
        dvideo_in,
        daudio_in,
        dbottle_in,
        video_qkv_grad,
        video_out_grad,
        audio_qkv_grad,
        audio_out_grad,
        gain_v[0],
        gain_a[0],
    )


def solution(mesh):
    split = Mesh(
        mesh.devices.reshape(2, 4, 4, 2, 2), ("fsdp_0", "fsdp_1", "fsdp_2", "rep_0", "rep_1")
    )
    return jax.shard_map(
        per_device,
        mesh=split,
        in_specs=(
            P(FSDP_REP, None, None),
            P(FSDP_REP, None, None),
            P(FSDP_REP, None, None),
            P(),
            P(),
            P(FSDP, None),
            P(FSDP, None),
            P(FSDP, None),
            P(FSDP, None),
            P(FSDP_REP, None, None),
            P(FSDP_REP, None, None),
            P(FSDP_REP, None, None),
        ),
        out_specs=(
            P(FSDP_REP, None, None),
            P(FSDP_REP, None, None),
            P(FSDP_REP, None, None),
            P(FSDP, None),
            P(FSDP, None),
            P(FSDP, None),
            P(FSDP, None),
            P(),
            P(),
        ),
        check_vma=False,
    )
```

```python
import functools

import jax
import jax.numpy as jnp
from jax import lax
from jax.experimental import pallas as pl
from jax.experimental.pallas import tpu as pltpu
from jax.sharding import Mesh
from jax.sharding import PartitionSpec as P

HEAD = 64
FSDP = ("fsdp_0", "fsdp_1", "fsdp_2")
FSDP_REP = ("fsdp_0", "fsdp_1", "fsdp_2", "rep_0", "rep_1")

f32 = jnp.float32
bf16 = jnp.bfloat16

RING = 4


def place_of(y, z, x, c):
    return (((y % 2) * RING + z) * RING + x) * 4 + (y // 2) * 2 + c


def pairs(move):
    out = []
    for y in range(RING):
        for z in range(RING):
            for x in range(RING):
                for c in range(2):
                    ny, nz, nx, nc = move(y, z, x, c)
                    out.append((place_of(y, z, x, c), place_of(ny % RING, nz % RING, nx % RING, nc)))
    return out


def send(value, move):
    return lax.ppermute(value, FSDP_REP, pairs(move))


def along_y(step):
    return lambda y, z, x, c: (y + step, z, x, c)


def along_last(step):
    return lambda y, z, x, c: (y, z + step * c, x + step * (1 - c), c)


def along_mid(step):
    return lambda y, z, x, c: (y, z + step * (1 - c), x + step * c, c)


def to_partner(y, z, x, c):
    return (y, z, x, 1 - c)


MID = ((0, 0), (0, 1), (-1, 0), (-1, 1), (1, 0), (1, 1), (2, 0), (2, 1))
LAST = (0, -1, 1, 2)


def coordinates():
    names = ("fsdp_1", "fsdp_2", "rep_1", "fsdp_0", "rep_0")
    return jnp.stack([lax.axis_index(name) for name in names]).astype(jnp.int32)


def block_row(where, block):
    z, x, c = where[0], where[1], where[2]
    last = LAST[block // 8]
    mid, half = MID[block % 8]
    zz = (z + mid * (1 - c) + last * c) & (RING - 1)
    xx = (x + last * (1 - c) + mid * c) & (RING - 1)
    return pl.multiple_of(half * 512 + zz * 128 + xx * 32, 32)


def in_vmem(n):
    return [pl.BlockSpec(memory_space=pltpu.VMEM)] * n


def in_smem():
    return pl.BlockSpec(memory_space=pltpu.SMEM)


def dot_nn(a, b):
    return lax.dot_general(a, b, (((1,), (0,)), ((), ())), preferred_element_type=f32)


def dot_nt(a, b):
    return lax.dot_general(a, b, (((1,), (1,)), ((), ())), preferred_element_type=f32)


def dot_tn(a, b):
    return lax.dot_general(a, b, (((0,), (0,)), ((), ())), preferred_element_type=f32)


def local_body(length, placed, where, own, peer, gain, *refs):
    size = own.shape[1]
    n_weights = 2 if placed else 16
    weights, refs = refs[:n_weights], refs[n_weights:]
    grads, refs = refs[:7], refs[7:]
    dh, gain_part, refs = refs[:2], refs[2], refs[3:]
    if placed:
        before, weights = weights[1], weights[:1]
    hidden, hidden_t, dyb, qkv, datt, att, dqkv, gqkv, gout, wqkv, wout = refs

    if placed:
        (full,) = weights
        base = pl.multiple_of(where[2] * 512, 512)

        def w_qkv(n):
            top = pl.multiple_of((n // 5) * 1024, 1024)
            return full[pl.ds(top, 1024), pl.ds(pl.multiple_of((n % 5) * 256, 256), 256)]

        def w_out(half):
            return full[pl.ds(1024 + base, 512), 256 + 512 * half : 768 + 512 * half]
    else:
        for n, ref in enumerate(weights):
            for k in range(ref.shape[0]):
                at = block_row(where, PIECE_BLOCKS[n][k])
                wqkv[pl.ds(at, 32), :] = ref[k, :, :1536]
                wout[pl.ds(at, 32), :] = ref[k, :, 1536:]

        def w_qkv(n):
            return wqkv[:, pl.ds(pl.multiple_of(n * 256, 256), 256)]

        def w_out(half):
            return wout[512 * half : 512 * half + 512, :]

    for b, pair in enumerate((own, peer)):
        z = pair[0].astype(f32)
        inverse = lax.rsqrt(jnp.mean(z * z, axis=1, keepdims=True) + 1e-06)
        hidden[b * size : (b + 1) * size, :] = (z * inverse * gain[...]).astype(bf16)
        dyb[b * size : (b + 1) * size, :] = pair[1]
    hidden_t[...] = hidden[...].T

    for n in range(6):
        qkv[:, 256 * n : 256 * n + 256] = dot_nn(hidden[...], w_qkv(n)).astype(bf16)

    datt[...] = (dot_nt(dyb[:, :512], w_out(0)) + dot_nt(dyb[:, 512:], w_out(1))).astype(bf16)

    scale = jnp.asarray(HEAD ** (-0.5), bf16)
    lane = lax.broadcasted_iota(jnp.int32, (size, 128), 1)
    key_at = lax.broadcasted_iota(jnp.int32, (size, size), 1)
    zero = jnp.zeros((), bf16)

    @pl.loop(0, 8, unroll=2)
    def _(n):
        r = pl.ds(pl.multiple_of((n // 4) * size, 16), size)
        at = pl.multiple_of((n % 4) * 128, 128)
        query = qkv[r, pl.ds(at, 128)]
        keyed = qkv[r, pl.ds(at + 512, 128)]
        valued = qkv[r, pl.ds(at + 1024, 128)]
        dout = datt[r, pl.ds(at, 128)]
        sums = [None] * 4
        for head in range(2):
            mine = (lane < HEAD) if head == 0 else (lane >= HEAD)
            q = jnp.where(mine, query * scale, zero)
            k = jnp.where(mine, keyed * scale, zero)
            v = jnp.where(mine, valued, zero)
            d = jnp.where(mine, dout, zero)
            score = dot_nt(q, keyed)
            score = jnp.where(key_at < length, score, -1e30)
            top = jnp.max(score, axis=1, keepdims=True)
            grown = jnp.exp(score - top)
            probs = grown * (1.0 / jnp.sum(grown, axis=1, keepdims=True))
            pb = probs.astype(bf16)
            dprob = dot_nt(d, valued)
            inner = jnp.sum(probs * dprob, axis=1, keepdims=True)
            dsb = (probs * (dprob - inner)).astype(bf16)
            parts = (dot_nn(pb, v), dot_nn(dsb, k), dot_tn(dsb, q), dot_tn(pb, d))
            sums = [p if t is None else t + p for t, p in zip(sums, parts)]
        att[r, pl.ds(at, 128)] = sums[0].astype(bf16)
        dqkv[r, pl.ds(at, 128)] = sums[1].astype(bf16)
        dqkv[r, pl.ds(at + 512, 128)] = sums[2].astype(bf16)
        dqkv[r, pl.ds(at + 1024, 128)] = sums[3].astype(bf16)

    att_t = att[...].T
    for half in range(2):
        gout[512 * half : 512 * half + 512, :] = dot_nn(
            att_t, dyb[:, 512 * half : 512 * half + 512]
        ).astype(bf16)

    gqkv[...] = dot_nn(hidden_t[...], dqkv[...]).astype(bf16)

    for n, ref in enumerate(grads):
        for k, block in enumerate(GRAD_BLOCKS[n]):
            at = block_row(where, block)
            ref[32 * k : 32 * k + 32, :1536] = gqkv[pl.ds(at, 32), :]
            ref[32 * k : 32 * k + 32, 1536:] = gout[pl.ds(at, 32), :]

    part = jnp.zeros((1, 1024), f32)
    for b, pair in enumerate((own, peer)):
        total = dot_nt(dqkv[b * size : (b + 1) * size, :256], w_qkv(0))
        for k in range(1, 6):
            total = total + dot_nt(dqkv[b * size : (b + 1) * size, k * 256 : k * 256 + 256], w_qkv(k))
        dh[b][...] = total
        z = pair[0].astype(f32)
        normed = z * lax.rsqrt(jnp.mean(z * z, axis=1, keepdims=True) + 1e-06)
        part = part + jnp.sum(total * normed, axis=0, keepdims=True)
    if placed:
        both = jnp.concatenate([before[...], part], 1)
        gain_part[...] = both
        for ref in grads[5:]:
            ref[128:144, :] = in_pieces(both)
    else:
        gain_part[...] = part


def in_pieces(value):
    first = value.astype(bf16).astype(f32)
    second = (value - first).astype(bf16).astype(f32)
    third = value - first - second
    row = lax.broadcasted_iota(jnp.int32, (16, value.shape[1]), 0)
    out = jnp.where(row == 0, first, jnp.where(row == 1, second, third))
    return jnp.where(row < 3, out, 0.0).astype(bf16)


def from_pieces(rows):
    rows = rows.astype(f32)
    return (rows[0:1] + rows[1:2]) + rows[2:3]


PIECE_BLOCKS = [(n, n + 1) for n in range(0, 32, 2)]
GRAD_BLOCKS = [tuple(range(8))]
for start in (8, 16, 24):
    GRAD_BLOCKS += [tuple(range(start, start + 4)), tuple(range(start + 4, start + 8))]


def local_compute(length, placed, where, own, peer, gain, weights):
    size = own.shape[1]
    total = 2 * size
    return pl.pallas_call(
        lambda *refs: local_body(length, placed, *refs),
        in_specs=[in_smem()] + in_vmem(3 + len(weights)),
        out_specs=in_vmem(10),
        out_shape=[jax.ShapeDtypeStruct((256, 2048), bf16)]
        + [jax.ShapeDtypeStruct((128, 2048), bf16)] * 4
        + [jax.ShapeDtypeStruct((144 if placed else 128, 2048), bf16)] * 2
        + [
            jax.ShapeDtypeStruct((size, 1024), f32),
            jax.ShapeDtypeStruct((size, 1024), f32),
            jax.ShapeDtypeStruct((1, 2048 if placed else 1024), f32),
        ],
        scratch_shapes=[
            pltpu.VMEM((total, 1024), bf16),
            pltpu.VMEM((1024, total), bf16),
            pltpu.VMEM((total, 1024), bf16),
            pltpu.VMEM((total, 1536), bf16),
            pltpu.VMEM((total, 512), bf16),
            pltpu.VMEM((total, 512), bf16),
            pltpu.VMEM((total, 1536), bf16),
            pltpu.VMEM((1024, 1536), bf16),
            pltpu.VMEM((1024, 512), bf16),
            pltpu.VMEM((16 if placed else 1024, 1536), bf16),
            pltpu.VMEM((16 if placed else 1024, 512), bf16),
        ],
        name="local_placed" if placed else "local_pieces",
    )(where, own, peer, gain.reshape(1, 1024), *weights)


def prepare(where, v_qkv, v_out, a_qkv, a_out, top, bottom, part):
    c, high = where[2], where[4]
    for k in range(3):
        at = pl.multiple_of(1024 * k + 512 * c, 512)
        top[:, 512 * k : 512 * k + 512] = v_qkv[:16, pl.ds(at, 512)]
        bottom[:, 512 * k : 512 * k + 512] = v_qkv[16:, pl.ds(at, 512)]
    top[:, 1536:] = v_out[:16, :]
    bottom[:, 1536:] = v_out[16:, :]
    flip = jnp.full((32, 1280), high, jnp.int32) == 1
    parts = [a_qkv[:, pl.ds(pl.multiple_of(1024 * k + 512 * c, 512), 512)] for k in range(3)]
    first = jnp.concatenate([parts[0], parts[1], parts[2][:, :256]], 1).astype(f32)
    second = jnp.concatenate([parts[2][:, 256:], a_out[...]], 1).astype(f32)
    part[...] = jnp.where(flip, second, first).astype(bf16)


def gather_by_rings(top, bottom):
    low = lax.axis_index("fsdp_0")
    c = lax.axis_index("rep_1")
    other_top = send(top, along_y(1))
    other_bottom = send(bottom, along_y(-1))
    shard = jnp.concatenate([top, bottom], 0)
    other = jnp.concatenate([other_top, other_bottom], 0)
    first = jnp.where(low == 0, shard[:, :1536], other[:, :1536])
    second = jnp.where(low == 0, other[:, :1536], shard[:, :1536])
    outw = jnp.where(low == c, shard[:, 1536:], other[:, 1536:])
    block = jnp.stack(
        [
            jnp.concatenate([first, outw[:, :512]], 1),
            jnp.concatenate([second, outw[:, 512:]], 1),
        ]
    )
    left = send(block, along_mid(1))
    right = send(block, along_mid(-1))
    far = send(left, along_mid(1))
    own = [block, left, right, far]
    from_left = [send(piece, along_last(1)) for piece in own]
    from_right = [send(piece, along_last(-1)) for piece in own]
    across = [send(piece, along_last(1)) for piece in from_left[:2]]
    across += [send(piece, along_last(-1)) for piece in from_right[2:]]
    return own + from_left + from_right + across


def add(*terms):
    total = terms[0].astype(f32)
    for term in terms[1:]:
        total = total + term.astype(f32)
    return total


def in_one_kernel(body, shapes, *args, scalars=None):
    specs = in_vmem(len(args))
    if scalars is not None:
        specs = [in_smem()] + specs
        args = (scalars,) + args
    return pl.pallas_call(
        body,
        in_specs=specs,
        out_specs=in_vmem(len(shapes)),
        out_shape=[jax.ShapeDtypeStruct(shape, dtype) for shape, dtype in shapes],
    )(*args)


def fold_far(right, left, up, down, right_out, left_out):
    right_out[:128, :] = add(right[...], up[:128, :]).astype(bf16)
    left_out[...] = add(left[...], down[:128, :]).astype(bf16)
    if right_out.shape[0] > 128:
        right_out[128:, :] = up[128:, :]


def first_steps(grads):
    own, left_a, left_b, right_a, right_b, far_a, far_b = grads
    up_far = send(far_a, along_last(1))
    down_far = send(far_b, along_last(-1))
    up_b = send(right_b, along_last(1))
    down_a = send(left_a, along_last(-1))
    return own, left_b, right_a, up_far, down_far, up_b, down_a


def second_steps(parts):
    own, left_b, right_a, up_far, down_far, up_b, down_a = parts
    right, left = in_one_kernel(
        fold_far, [(up_far.shape, bf16), ((128, 2048), bf16)], right_a, left_b, up_far, down_far
    )
    up_a = send(right, along_last(1))
    down_b = send(left, along_last(-1))
    return own, up_a, up_b, down_a, down_b


def ring_sum(own, left, right, far):
    return (own + far) + (left + right)


def fold_sum(own, up_a, up_b, down_a, down_b, out):
    out[:128, :] = add(own[:128, :], up_a[:128, :], down_a[:128, :]).astype(bf16)
    out[128:, :] = add(own[128:, :], up_b[...], down_b[...]).astype(bf16)


def fold_last(video, own, up_a, up_b, down_a, down_b, gain, up_far, down_far,
              right, left, across, home, gain_out):
    for s in range(2):
        for j in range(8):
            u, d, at = (up_a, down_a, 32 * j) if j < 4 else (up_b, down_b, 32 * j - 128)
            if s == 0:
                total = video[32 * j : 32 * j + 32, :].astype(f32)
            else:
                total = add(own[32 * j : 32 * j + 32, :], u[at : at + 32, :], d[at : at + 32, :])
            row = 64 * s + 32 * (j % 2)
            (home, left, right, across)[j // 2][row : row + 32, :] = total.astype(bf16)
    total = ring_sum(
        gain[...],
        from_pieces(up_far[128:144, :]),
        from_pieces(down_far[128:144, :]),
        from_pieces(up_a[128:144, :]),
    )
    gain_out[...] = total
    for ref in (right, left, across):
        ref[128:144, :] = in_pieces(total)


def fold_mid(where, home, gain, up, down, far, same, cross, gain_out):
    low = where[3]
    for s in range(2):
        first, second = (
            add(home[r, :], far[r, :], up[r, :], down[r, :]).astype(bf16)
            for r in (pl.ds(64 * s, 32), pl.ds(64 * s + 32, 32))
        )
        r = slice(32 * s, 32 * s + 32)
        flip = jnp.full((32, 1536), low, jnp.int32) == 1
        a, b = first[:, :1536].astype(f32), second[:, :1536].astype(f32)
        same[r, :1536] = jnp.where(flip, b, a).astype(bf16)
        cross[r, :1536] = jnp.where(flip, a, b).astype(bf16)
        for ref in (same, cross):
            ref[r, 1536:2048] = first[:, 1536:]
            ref[r, 2048:] = second[:, 1536:]
    total = ring_sum(
        gain[...],
        from_pieces(up[128:144, :]),
        from_pieces(down[128:144, :]),
        from_pieces(far[128:144, :]),
    )
    gain_out[...] = total
    for ref in (same, cross):
        ref[64:72, :2048] = in_pieces(total)[:8]
        ref[64:72, 2048:] = jnp.zeros((8, 512), bf16)


def fold_y(count, same, up, down, far, gain, out):
    total = add(same[:64, :], far[:64, :]) + add(up[:64, :], down[:64, :])
    out[:64, :] = total / count
    total = ring_sum(
        gain[...],
        from_pieces(up[64:72, :2048]),
        from_pieces(down[64:72, :2048]),
        from_pieces(far[64:72, :2048]),
    )
    out[64:72, :2048] = jnp.broadcast_to(total, (8, 2048))
    out[64:72, 2048:] = jnp.zeros((8, 512), f32)


def spread(count, where, mine, peer, v_qkv, v_out, a_qkv, a_out, gain_v, gain_a):
    c, low = where[2], where[3]
    for s, (qkv, out) in enumerate(((v_qkv, v_out), (a_qkv, a_out))):
        r = slice(32 * s, 32 * s + 32)
        for k in range(3):
            at = pl.multiple_of(1024 * k + 512 * c, 512)
            qkv[:, pl.ds(at, 512)] = mine[r, 512 * k : 512 * k + 512]
            at = pl.multiple_of(1024 * k + 512 * (1 - c), 512)
            qkv[:, pl.ds(at, 512)] = peer[r, 512 * k : 512 * k + 512]
        here = jnp.full((32, 1024), (low == c).astype(jnp.int32), jnp.int32) == 1
        out[...] = jnp.where(here, mine[r, 1536:], peer[r, 1536:])
    total = (mine[64:72, :2048] + peer[64:72, :2048]) / count
    gain_v[...] = total[0:1, :1024]
    gain_a[...] = total[0:1, 1024:]


def last_steps(video, audio, audio_parts, gain, where, count):
    audio_far = audio_parts[3:5]
    (video_sum,) = in_one_kernel(fold_sum, [((256, 2048), bf16)], *video)
    right, left, across, home, gain = in_one_kernel(
        fold_last,
        [((144, 2048), bf16)] * 3 + [((128, 2048), bf16), ((1, 2048), f32)],
        video_sum,
        *audio,
        gain,
        *audio_far,
    )
    far = send(across, along_mid(2))
    up = send(right, along_mid(1))
    down = send(left, along_mid(-1))
    same, cross, gain = in_one_kernel(
        fold_mid,
        [((72, 2560), bf16)] * 2 + [((1, 2048), f32)],
        home,
        gain,
        up,
        down,
        far,
        scalars=where,
    )
    far = send(same, along_y(2))
    up = send(cross, along_y(1))
    down = send(cross, along_y(-1))
    (total,) = in_one_kernel(
        functools.partial(fold_y, count), [((72, 2560), f32)], same, up, down, far, gain
    )
    peer = send(total, to_partner)
    return in_one_kernel(
        functools.partial(spread, count),
        [((32, 3072), f32), ((32, 1024), f32)] * 2 + [((1, 1024), f32)] * 2,
        total,
        peer,
        scalars=where,
    )


def clip_pair(tokens, bottle, d_tokens, d_bottle):
    half = (d_bottle.astype(f32) * 0.5).astype(bf16)
    pad = jnp.zeros((-(tokens.shape[0] + bottle.shape[0]) % 16, 1024), bf16)
    own = jnp.stack(
        [jnp.concatenate([tokens, bottle, pad], 0), jnp.concatenate([d_tokens, half, pad], 0)]
    )
    return own, send(own, to_partner)


def finish(own, gain, dh, dh_peer):
    from_peer = send(dh_peer, to_partner)
    dhidden = dh + from_peer
    z = own[0].astype(f32)
    inverse = lax.rsqrt(jnp.mean(z * z, axis=1, keepdims=True) + 1e-06)
    normed = z * inverse
    dnorm = dhidden * gain
    d_out = own[1].astype(f32)
    mean = jnp.mean(dnorm * normed, axis=1, keepdims=True)
    return d_out + inverse * (dnorm - normed * mean)


def per_device(
    video_in,
    audio_in,
    bottle_in,
    video_gain,
    audio_gain,
    video_qkv,
    video_out,
    audio_qkv,
    audio_out,
    grad_video,
    grad_audio,
    grad_bottle,
):
    count = float(video_in.shape[0] * lax.axis_size(FSDP_REP))
    where = coordinates()
    video_len = video_in.shape[1]
    audio_len = audio_in.shape[1]
    bottle_len = bottle_in.shape[1]
    top, bottom, part = in_one_kernel(
        prepare,
        [((16, 2560), bf16)] * 2 + [((32, 1280), bf16)],
        video_qkv,
        video_out,
        audio_qkv,
        audio_out,
        scalars=where,
    )
    aweights = lax.all_gather(part, ("rep_0",) + FSDP, axis=0, tiled=True)
    vweights = gather_by_rings(top, bottom)
    vown, vpeer = clip_pair(video_in[0], bottle_in[0], grad_video[0], grad_bottle[0])
    aown, apeer = clip_pair(audio_in[0], bottle_in[0], grad_audio[0], grad_bottle[0])
    vpeer, apeer = lax.optimization_barrier((vpeer, apeer))
    *grads, dh_video, dh_video_peer, gain_v = local_compute(
        video_len + bottle_len, False, where, vown, vpeer, video_gain, vweights
    )
    video_parts = first_steps(grads)
    *grads, dh_audio, dh_audio_peer, gain = local_compute(
        audio_len + bottle_len,
        True,
        where,
        aown,
        apeer,
        audio_gain,
        [aweights, gain_v],
    )
    audio_parts = first_steps(grads)
    video = second_steps(video_parts)
    audio = second_steps(audio_parts)
    (
        video_qkv_grad,
        video_out_grad,
        audio_qkv_grad,
        audio_out_grad,
        gain_v,
        gain_a,
    ) = last_steps(video, audio, audio_parts, gain, where, count)
    dz_video = finish(vown, video_gain, dh_video, dh_video_peer)
    dz_audio = finish(aown, audio_gain, dh_audio, dh_audio_peer)
    video_end = video_len + bottle_len
    audio_end = audio_len + bottle_len
    dvideo_in = dz_video[None, :video_len].astype(bf16)
    daudio_in = dz_audio[None, :audio_len].astype(bf16)
    dbottle_in = dz_video[None, video_len:video_end] + dz_audio[None, audio_len:audio_end]
    dbottle_in = dbottle_in.astype(bf16)
    return (
        dvideo_in,
        daudio_in,
        dbottle_in,
        video_qkv_grad,
        video_out_grad,
        audio_qkv_grad,
        audio_out_grad,
        gain_v[0],
        gain_a[0],
    )


def solution(mesh):
    split = Mesh(
        mesh.devices.reshape(2, 4, 4, 2, 2), ("fsdp_0", "fsdp_1", "fsdp_2", "rep_0", "rep_1")
    )
    return jax.shard_map(
        per_device,
        mesh=split,
        in_specs=(
            P(FSDP_REP, None, None),
            P(FSDP_REP, None, None),
            P(FSDP_REP, None, None),
            P(),
            P(),
            P(FSDP, None),
            P(FSDP, None),
            P(FSDP, None),
            P(FSDP, None),
            P(FSDP_REP, None, None),
            P(FSDP_REP, None, None),
            P(FSDP_REP, None, None),
        ),
        out_specs=(
            P(FSDP_REP, None, None),
            P(FSDP_REP, None, None),
            P(FSDP_REP, None, None),
            P(FSDP, None),
            P(FSDP, None),
            P(FSDP, None),
            P(FSDP, None),
            P(),
            P(),
        ),
        check_vma=False,
    )
```
